32 devices in a mesh: gy: 8 (over y, x, core), gx: 4 (over z).
Axes of the slice: x: 2, y: 2, z: 4, core: 2. Of those that a mesh axis runs over, the one named last changes fastest.
Arguments:
- tracer: float32 [8, 1024, 1024], P(None, 'gy', 'gx'), may hold values from -6 to 6
- east_speed: float32 [8, 1024, 1024], P(None, 'gy', 'gx'), may hold values from -0.25 to 0.25
- north_speed: float32 [8, 1024, 1024], P(None, 'gy', 'gx'), may hold values from -0.25 to 0.25
- columns: int32 [1024, 1024], P('gy', 'gx'), may hold values from 0 to 8
- thickness: float32 [8], replicated, may hold values from 0.5 to 2
- surface_flux: float32 [1024, 1024], P('gy', 'gx'), may hold values from -6 to 6
- helm: float32 [1024, 1024], P('gy', 'gx'), may hold values from 0.2 to 4
Outputs:
- tracer_new: float32 [8, 1024, 1024], P(None, 'gy', 'gx')
- heights: float32 [1024, 1024], P('gy', 'gx')
The draws below stay inside these ranges and needn't reach their ends.
Inputs may be any that keep to these rules, and one draw needn't show every extreme that they name: `columns`: ocean levels per column; 0 means land.
All inputs are finite; a program needn't handle non-finite values.
Results may differ from the reference program's by a relative error of at most 0.0001.
Values sent between devices are 32-bit elements; how exact they have to be, the bound alone decides.
A program may use at most 64 MiB of HBM per device.

```python
import math
import jax
import jax.numpy as jnp
from jax import lax

K = 8
TSTEPS = 2
ITERS = 3
NY = 1024
NX = 1024


def plant(entries, own_key, smallest, top_value):
    shape = entries.shape
    index_at = [jax.random.randint(jax.random.fold_in(own_key, axis), (), 0, shape[axis]) for axis in range(len(shape))]
    entries = entries.at[tuple(index_at)].set(smallest)
    longest = shape.index(max(shape))
    index_at[longest] = (index_at[longest] + 1) % shape[longest]
    return entries.at[tuple(index_at)].set(top_value)


def block_levels(stream_key, shape, split, least, top_value):
    def one(dim, blocks):
        steps = jax.random.uniform(jax.random.fold_in(jax.random.fold_in(stream_key, 6), dim), (blocks,), jnp.float32, least / len(split), top_value / len(split))
        return jnp.repeat(jnp.exp(steps), shape[dim] // blocks).reshape((-1,) + (1,) * (len(shape) - dim - 1))

    loudness = one(*split[0])
    for cut in split[1:]:
        loudness = loudness * one(*cut)
    return loudness


def normal_values(own_key, extent, width, bound, pieces=(), kind=jnp.bfloat16):
    drawn = width * jax.random.normal(own_key, extent, jnp.float32)
    if pieces:
        drawn = drawn * block_levels(own_key, extent, pieces, -0.22, 0.18)
    return jnp.clip(drawn, -bound, bound).astype(kind)


def setup_inputs(seed: int = 0) -> dict:
    arg_keys = jax.random.split(jax.random.key(seed), 8)
    return {
        "tracer": normal_values(arg_keys[0], (K, NY, NX), 1.0, 6.0, ((1, 8), (2, 4)), jnp.float32),
        "east_speed": jnp.clip(jax.random.uniform(arg_keys[1], (K, NY, NX), jnp.float32, -0.25, 0.25) * block_levels(arg_keys[1], (K, NY, NX), ((1, 8), (2, 4)), -0.4, 0.0), -0.25, 0.25),
        "north_speed": jnp.clip(jax.random.uniform(arg_keys[2], (K, NY, NX), jnp.float32, -0.25, 0.25) * block_levels(arg_keys[2], (K, NY, NX), ((1, 8), (2, 4)), -0.4, 0.0), -0.25, 0.25),
        "columns": plant(jax.random.randint(arg_keys[3], (NY, NX), 0, K + 1), jax.random.fold_in(arg_keys[3], 1), 0, K).astype(jnp.int32),
        "thickness": jnp.clip(jnp.exp(jax.random.uniform(arg_keys[4], (K,), jnp.float32, math.log(0.5), math.log(2.0))), 0.5, 2.0),
        "surface_flux": normal_values(arg_keys[5], (NY, NX), 1.0, 6.0, ((0, 8), (1, 4)), jnp.float32),
        "helm": jnp.clip(jnp.exp(math.log(4.0) - 2.9957323 * jax.random.uniform(arg_keys[6], (NY, NX), jnp.float32) ** block_levels(arg_keys[6], (NY, NX), ((0, 8), (1, 4)), -0.2, 0.2)), 0.2, 4.0),
    }


def upwind(speed, behind, ahead):
    return jnp.maximum(speed, 0.0) * behind + jnp.minimum(speed, 0.0) * ahead


def advect(current, east_speed, north_speed, ocean):
    tracer_east = jnp.roll(current, -1, axis=2)
    ocean_east = jnp.roll(ocean, -1, axis=2)
    tracer_north = jnp.pad(current[:, 1:, :], ((0, 0), (0, 1), (0, 0)))
    ocean_north = jnp.pad(ocean[:, 1:, :], ((0, 0), (0, 1), (0, 0)))
    flux_east = ocean * ocean_east * upwind(east_speed, current, tracer_east)
    flux_north = ocean * ocean_north * upwind(north_speed, current, tracer_north)
    flux_west = jnp.roll(flux_east, 1, axis=2)
    flux_south = jnp.pad(flux_north[:, :-1, :], ((0, 0), (1, 0), (0, 0)))
    return current - (flux_east - flux_west + flux_north - flux_south)


def neighbour(source, row_step, col_step):
    moved = jnp.roll(source, -col_step, axis=1)
    if row_step == 1:
        moved = jnp.pad(moved[1:], ((0, 1), (0, 0)))
    elif row_step == -1:
        moved = jnp.pad(moved[:-1], ((1, 0), (0, 0)))
    return moved


def nine_point(source, wet, diagonal_term):
    weighted = wet * source
    edges = neighbour(weighted, 0, 1) + neighbour(weighted, 0, -1) + neighbour(weighted, 1, 0) + neighbour(weighted, -1, 0)
    corners = neighbour(weighted, 1, 1) + neighbour(weighted, 1, -1) + neighbour(weighted, -1, 1) + neighbour(weighted, -1, -1)
    return diagonal_term * source - wet * (edges + 0.5 * corners)


def reference(tracer, east_speed, north_speed, columns, thickness, surface_flux, helm):
    depth = lax.broadcasted_iota(jnp.int32, tracer.shape, 0)
    ocean = (depth < columns[None]).astype(jnp.float32)
    current = tracer
    for section_index in range(TSTEPS):
        current = advect(current, east_speed, north_speed, ocean)
    forcing = surface_flux + jnp.sum(thickness[:, None, None] * ocean * current, axis=0)
    wet = ocean[0]
    diagonal_term = 6.0 + helm
    heights = jnp.zeros_like(forcing)
    residual = forcing
    scaled = residual / diagonal_term
    direction = scaled
    product_now = jnp.sum(residual * scaled)
    for iteration in range(ITERS):
        applied = nine_point(direction, wet, diagonal_term)
        step_size = product_now / jnp.sum(direction * applied)
        heights = heights + step_size * direction
        residual = residual - step_size * applied
        scaled = residual / diagonal_term
        product_next = jnp.sum(residual * scaled)
        direction = scaled + (product_next / product_now) * direction
        product_now = product_next
    return current, heights
```

```python
import functools

import jax
import jax.numpy as jnp
from jax import lax
from jax.experimental import pallas as pl
from jax.experimental.pallas import tpu as pltpu
from jax.sharding import PartitionSpec as P

TSTEPS = 2
ITERS = 3
MESH = pl.DeviceIdType.MESH
SUB = 8
LANE = 128
AROUND = ((1, 0), (-1, 0), (0, 1), (0, -1), (1, 1), (1, -1), (-1, 1), (-1, -1))


def roll(array, shift, axis):
    shift = shift % array.shape[axis]
    return pltpu.roll(array, shift, axis) if shift else array


def iota(shape, dim):
    return lax.broadcasted_iota(jnp.int32, shape, dim)


def kernel(
    ny,
    nx,
    tracer_ref,
    east_ref,
    north_ref,
    columns_ref,
    thick_hbm,
    surface_ref,
    helm_ref,
    tracer_out,
    heights_out,
    c_ext,
    e_ext,
    n_ext,
    col_in,
    surf_in,
    flat_ext,
    face_levels,
    pack,
    to_left,
    to_right,
    from_left,
    from_right,
    corner_recv,
    up_send,
    down_send,
    up_recv,
    down_recv,
    forcing,
    start_vec,
    flat_pack,
    edge_pack,
    row_recv,
    edge_recv,
    edge_corner_recv,
    part,
    slots,
    thickness_ref,
    in_sem,
    out_sem,
    send_sem,
    recv_sem,
    sum_send_sem,
    sum_recv_sem,
):
    levels, rows, cols = tracer_ref.shape
    ext_rows, ext_cols = rows + SUB, cols + LANE
    my_y, my_x = lax.axis_index("gy"), lax.axis_index("gx")
    count = ny * nx
    my_id = my_y * nx + my_x

    def place(offset):
        target = lax.rem(my_id + offset, count)
        return (target // nx, lax.rem(target, nx))

    def near(dy, dx):
        return (lax.rem(my_y + dy + ny, ny), lax.rem(my_x + dx + nx, nx))

    loads = [
        pltpu.make_async_copy(columns_ref, col_in, in_sem.at[0]),
        pltpu.make_async_copy(helm_ref, flat_ext.at[1, 0:rows, 0:cols], in_sem.at[1]),
        pltpu.make_async_copy(tracer_ref, c_ext.at[:, 0:rows, 0:cols], in_sem.at[2]),
        pltpu.make_async_copy(east_ref, e_ext.at[:, 0:rows, 0:cols], in_sem.at[3]),
        pltpu.make_async_copy(north_ref, n_ext.at[:, 0:rows, 0:cols], in_sem.at[4]),
        pltpu.make_async_copy(surface_ref, surf_in, in_sem.at[5]),
        pltpu.make_async_copy(thick_hbm, thickness_ref, in_sem.at[6]),
    ]
    for load in loads:
        load.start()
    barrier = pltpu.get_barrier_semaphore()
    for offset in range(1, count):
        pl.semaphore_signal(barrier, inc=1, device_id=place(offset), device_id_type=MESH)
    for load in loads:
        load.wait()

    fields = (c_ext, e_ext, n_ext)
    flat_ext[0, 0:rows, 0:cols] = col_in[...].astype(jnp.float32)

    lane_full = iota((rows, LANE), 1)
    lane_half = lane_full < LANE // 2
    group = lane_full // 4

    def both_edges(ref, index):
        return jnp.where(lane_half, ref[index, 0:rows, 0:LANE], ref[index, 0:rows, cols - LANE : cols])

    sources = [(fields[f], k, f) for k in range(levels) for f in range(3)]
    sources += [(flat_ext, 0, 3), (flat_ext, 1, 4)]
    packed = jnp.zeros((rows, LANE), jnp.float32)
    for slot, (ref, index, _) in enumerate(sources):
        packed = jnp.where(group == slot, roll(both_edges(ref, index), 4 * slot + 2, 1), packed)
    pack[...] = packed
    turned = packed.T
    sub_rows = iota((SUB, rows), 0) % 4 < 2
    for p in range(to_left.shape[0]):
        one, two = turned[2 * SUB * p :][:SUB], turned[2 * SUB * p + SUB :][:SUB]
        to_right[p] = jnp.where(sub_rows, one, roll(two, 2, 0))
        to_left[p] = jnp.where(sub_rows, roll(two, -2, 0), one)

    sub = iota((SUB, cols), 0)
    for k in range(levels):
        quads = [(ref, k) for ref in fields] + [(flat_ext, min(k, 1))]
        up = jnp.zeros((SUB, cols), jnp.float32)
        down = jnp.zeros((SUB, cols), jnp.float32)
        for f, (ref, index) in enumerate(quads):
            mine = sub // 2 == f
            up = jnp.where(mine, roll(ref[index, rows - SUB : rows, 0:cols], 2 * f + 2, 0), up)
            down = jnp.where(mine, roll(ref[index, 0:SUB, 0:cols], 2 * f, 0), down)
        up_send[k] = up
        down_send[k] = down

    pl.semaphore_wait(barrier, count - 1)

    first_rows, last_rows = pl.ds(0, SUB), pl.ds(rows - SUB, SUB)
    first = [
        (up_send, up_recv),
        (down_send, down_recv),
        (to_right, from_left),
        (to_left, from_right),
        (pack.at[last_rows], corner_recv.at[0]),
        (pack.at[last_rows], corner_recv.at[1]),
        (pack.at[first_rows], corner_recv.at[2]),
        (pack.at[first_rows], corner_recv.at[3]),
    ]

    def exchange(pairs, base):
        copies = []
        for which, (source, target) in enumerate(pairs):
            copies.append(
                pltpu.make_async_remote_copy(
                    src_ref=source,
                    dst_ref=target,
                    send_sem=send_sem.at[base + which],
                    recv_sem=recv_sem.at[base + which],
                    device_id=near(*AROUND[which]),
                    device_id_type=MESH,
                )
            )
        for copy in reversed(copies):
            copy.start()
        return copies

    copies = exchange(first, 0)
    for copy in copies:
        copy.wait_recv()

    pieces = []
    for p in range(to_left.shape[0]):
        x, y = from_left[p], from_right[p]
        pieces.append(jnp.where(sub_rows, x, y))
        pieces.append(jnp.where(sub_rows, roll(x, -2, 0), roll(y, 2, 0)))
    spare = LANE - 2 * SUB * to_left.shape[0]
    if spare:
        pieces.append(jnp.zeros((spare, rows), jnp.float32))
    sides = jnp.concatenate(pieces, axis=0).T
    small_right = (iota((SUB, LANE), 1) % 4) >= 2
    small_below = iota((SUB, LANE), 0) < SUB // 2
    south = jnp.where(small_right, corner_recv[1], corner_recv[0])
    north = jnp.where(small_right, corner_recv[3], corner_recv[2])
    corner = jnp.where(small_below, north, south)
    for slot, (ref, index, _) in enumerate(sources):
        ref[index, 0:rows, cols:ext_cols] = roll(sides, -4 * slot - 2, 1)
        ref[index, rows:ext_rows, cols:ext_cols] = roll(corner, -4 * slot - 2, 1)
    for k in range(levels):
        quads = [(ref, k) for ref in fields] + ([(flat_ext, k)] if k < 2 else [])
        for f, (ref, index) in enumerate(quads):
            ref[index, rows:ext_rows, 0:cols] = jnp.where(
                sub < SUB // 2,
                roll(down_recv[k], -2 * f, 0),
                roll(up_recv[k], -2 * f - 2, 0),
            )

    row_ids = iota((SUB, ext_cols), 0)
    beyond = (row_ids >= SUB // 2) & (my_y == 0) | (row_ids < SUB // 2) & (my_y == ny - 1)
    flat_ext[0, rows:ext_rows] = jnp.where(beyond, 0.0, flat_ext[0, rows:ext_rows])

    forcing[...] = surf_in[...]

    depth = flat_ext[0]
    face_levels[0] = jnp.minimum(depth, roll(depth, -1, 1))
    face_levels[1] = jnp.minimum(depth, roll(depth, -1, 0))

    def level(k, carry):
        below = lax.convert_element_type(k, jnp.float32)
        east = jnp.where(face_levels[0] > below, e_ext[k], 0.0)
        nort = jnp.where(face_levels[1] > below, n_ext[k], 0.0)
        current = c_ext[k]
        for _ in range(TSTEPS):
            flux_east = east * jnp.where(east > 0.0, current, roll(current, -1, 1))
            flux_north = nort * jnp.where(nort > 0.0, current, roll(current, -1, 0))
            current = current - (
                flux_east - roll(flux_east, 1, 1) + flux_north - roll(flux_north, 1, 0)
            )
        tracer_out[k] = current[0:rows, 0:cols]
        open_here = flat_ext[0, 0:rows, 0:cols] > below
        forcing[...] += jnp.where(open_here, thickness_ref[k] * current[0:rows, 0:cols], 0.0)
        return carry

    lax.fori_loop(0, levels, level, 0, unroll=2)

    diagonal = 6.0 + flat_ext[1, 0:rows, 0:cols]
    wet = jnp.where(flat_ext[0, 0:rows, 0:cols] > 0.0, 1.0, 0.0)
    z0 = forcing[...] / diagonal
    y0 = wet * z0
    start_vec[0:rows, 0:cols] = y0
    edges = jnp.where(lane_half, y0[:, 0:LANE], y0[:, cols - LANE : cols])
    flat_pack[...] = edges
    edge_pack[...] = edges.T
    last_lanes = pl.ds(LANE - SUB, SUB)
    second = [
        (start_vec.at[last_rows, pl.ds(0, cols)], row_recv.at[0]),
        (start_vec.at[first_rows, pl.ds(0, cols)], row_recv.at[1]),
        (edge_pack.at[last_lanes], edge_recv.at[0]),
        (edge_pack.at[first_rows], edge_recv.at[1]),
        (flat_pack.at[last_rows], edge_corner_recv.at[0]),
        (flat_pack.at[last_rows], edge_corner_recv.at[1]),
        (flat_pack.at[first_rows], edge_corner_recv.at[2]),
        (flat_pack.at[first_rows], edge_corner_recv.at[3]),
    ]
    more = exchange(second, len(AROUND))
    for copy in more:
        copy.wait_recv()

    turned = jnp.concatenate(
        [edge_recv[1], jnp.zeros((LANE - 2 * SUB, rows), jnp.float32), edge_recv[0]], axis=0
    )
    lane_small = iota((SUB, LANE), 1) < LANE // 2
    south = jnp.where(lane_small, edge_corner_recv[1], edge_corner_recv[0])
    north = jnp.where(lane_small, edge_corner_recv[3], edge_corner_recv[2])
    for copy in more:
        copy.wait_send()
    start_vec[0:rows, cols:ext_cols] = turned.T
    start_vec[rows:ext_rows, cols:ext_cols] = jnp.where(small_below, north, south)
    start_vec[rows:ext_rows, 0:cols] = jnp.where(sub < SUB // 2, row_recv[1], row_recv[0])
    start_vec[rows:ext_rows] = jnp.where(beyond, 0.0, start_vec[rows:ext_rows])

    scale = jnp.where(flat_ext[0] > 0.0, 1.0 / (6.0 + flat_ext[1]), 0.0)

    def off_diagonal(vector):
        across = roll(vector, 1, 1) + roll(vector, -1, 1)
        mixed = vector + 0.5 * across
        return scale * (across + roll(mixed, 1, 0) + roll(mixed, -1, 0))

    z1_ext = off_diagonal(start_vec[...])
    z2_ext = off_diagonal(z1_ext)
    z3_ext = off_diagonal(z2_ext)
    z1, z2, z3 = (z[0:rows, 0:cols] for z in (z1_ext, z2_ext, z3_ext))

    def partial(values):
        folded = jnp.sum(values, axis=0, keepdims=True)
        return sum(folded[:, i : i + LANE] for i in range(0, cols, LANE))

    d0, d1, d2 = (diagonal * z for z in (z0, z1, z2))
    sums = [partial(v) for v in (d0 * z0, d0 * z1, d1 * z1, d1 * z2, d2 * z2, d2 * z3)]
    folded = jnp.concatenate(sums + [jnp.zeros((SUB - len(sums), LANE), jnp.float32)], axis=0)
    for shift in (64, 32, 16):
        folded = folded + roll(folded, shift, 1)
    own = iota((SUB, LANE), 1) // (LANE // SUB) == iota((SUB, LANE), 0)
    part[...] = jnp.sum(jnp.where(own, folded, 0.0), axis=0, keepdims=True)

    for offset in range(1, count):
        pltpu.make_async_remote_copy(
            src_ref=part,
            dst_ref=slots.at[offset - 1],
            send_sem=sum_send_sem,
            recv_sem=sum_recv_sem,
            device_id=place(offset),
            device_id_type=MESH,
        ).start()
    everything = pltpu.make_async_remote_copy(
        src_ref=slots,
        dst_ref=slots,
        send_sem=sum_send_sem,
        recv_sem=sum_recv_sem,
        device_id=place(1),
        device_id_type=MESH,
    )
    everything.wait_recv()
    total = jnp.sum(slots[...], axis=0) + part[...]
    total = jnp.sum(jnp.where(own, total, 0.0), axis=1, keepdims=True)
    moment = [total[i : i + 1, :] for i in range(2 * ITERS)]

    def inner(a, b):
        return sum(x * y * moment[i + j] for i, x in enumerate(a) for j, y in enumerate(b))

    def ratio(top, bottom):
        good = bottom > 0.0
        return jnp.where(good, top / jnp.where(good, bottom, 1.0), 0.0)

    one, zero = jnp.ones((1, 1), jnp.float32), jnp.zeros((1, 1), jnp.float32)
    scaled, direction, height = [one], [one], [zero] * ITERS
    product_now = moment[0]
    for iteration in range(ITERS):
        low, high = direction + [zero], [zero] + direction
        applied = [a - b for a, b in zip(low, high)]
        step_size = ratio(product_now, inner(direction, applied))
        for i, x in enumerate(direction):
            height[i] = height[i] + step_size * x
        if iteration + 1 < ITERS:
            scaled = [a - step_size * b for a, b in zip(scaled + [zero], applied)]
            product_next = jnp.maximum(inner(scaled, scaled), 0.0)
            factor = ratio(product_next, product_now)
            direction = [a + factor * b for a, b in zip(scaled, low)]
            product_now = product_next
    heights_out[...] = height[0] * z0 + height[1] * z1 + height[2] * z2

    everything.wait_send()
    for copy in copies:
        copy.wait_send()


def hand_on(tracer_ref, heights_ref, tracer_out, heights_out, save):
    levels = tracer_ref.shape[0]
    stages = [(heights_ref, heights_out)]
    stages += [(tracer_ref.at[k], tracer_out.at[k]) for k in range(levels)]
    saves = [pltpu.make_async_copy(a, b, save.at[i]) for i, (a, b) in enumerate(stages)]
    for copy in saves:
        copy.start()
    for copy in saves:
        copy.wait()


def on_device(ny, nx, tracer, east_speed, north_speed, columns, thickness, surface_flux, helm):
    levels, rows, cols = tracer.shape
    ext = (rows + SUB, cols + LANE)
    hbm = pl.BlockSpec(memory_space=pl.ANY)
    vmem = pl.BlockSpec(memory_space=pltpu.VMEM)
    f32 = jnp.float32
    dma = pltpu.SemaphoreType.DMA
    pairs = pl.cdiv(4 * (3 * levels + 2), 2 * SUB)
    scratch = [
        pltpu.VMEM((levels, *ext), f32),
        pltpu.VMEM((levels, *ext), f32),
        pltpu.VMEM((levels, *ext), f32),
        pltpu.VMEM((rows, cols), jnp.int32),
        pltpu.VMEM((rows, cols), f32),
        pltpu.VMEM((2, *ext), f32),
        pltpu.VMEM((2, *ext), f32),
        pltpu.VMEM((rows, LANE), f32),
        *[pltpu.VMEM((pairs, SUB, rows), f32)] * 4,
        pltpu.VMEM((4, SUB, LANE), f32),
        pltpu.VMEM((levels, SUB, cols), f32),
        pltpu.VMEM((levels, SUB, cols), f32),
        pltpu.VMEM((levels, SUB, cols), f32),
        pltpu.VMEM((levels, SUB, cols), f32),
        pltpu.VMEM((rows, cols), f32),
        pltpu.VMEM(ext, f32),
        pltpu.VMEM((rows, LANE), f32),
        pltpu.VMEM((LANE, rows), f32),
        pltpu.VMEM((2, SUB, cols), f32),
        pltpu.VMEM((2, SUB, rows), f32),
        pltpu.VMEM((4, SUB, LANE), f32),
        pltpu.VMEM((1, LANE), f32),
        pltpu.VMEM((ny * nx - 1, 1, LANE), f32),
        pltpu.SMEM((levels,), f32),
        dma((7,)),
        dma,
        dma((2 * len(AROUND),)),
        dma((2 * len(AROUND),)),
        dma,
        dma,
    ]
    results = pl.pallas_call(
        functools.partial(kernel, ny, nx),
        out_shape=(
            pltpu.VMEM((levels, rows, cols), f32),
            pltpu.VMEM((rows, cols), f32),
        ),
        in_specs=[hbm, hbm, hbm, hbm, hbm, hbm, hbm],
        out_specs=(vmem, vmem),
        scratch_shapes=scratch,
        compiler_params=pltpu.CompilerParams(collective_id=0, has_side_effects=True),
    )(tracer, east_speed, north_speed, columns, thickness, surface_flux, helm)
    return pl.pallas_call(
        hand_on,
        out_shape=tuple(jax.ShapeDtypeStruct(r.shape, f32) for r in results),
        in_specs=[vmem, vmem],
        out_specs=(hbm, hbm),
        scratch_shapes=[dma((levels + 1,))],
    )(*[pltpu.with_memory_space_constraint(r, pltpu.VMEM) for r in results])


def solution(mesh):
    spec = P(None, "gy", "gx")
    flat = P("gy", "gx")
    return jax.shard_map(
        functools.partial(on_device, mesh.shape["gy"], mesh.shape["gx"]),
        mesh=mesh,
        in_specs=(spec, spec, spec, flat, P(), flat, flat),
        out_specs=(spec, flat),
        check_vma=False,
    )
```

```python
import functools

import jax
import jax.numpy as jnp
from jax import lax
from jax.experimental import pallas as pl
from jax.experimental.pallas import tpu as pltpu
from jax.sharding import PartitionSpec as P

TSTEPS = 2
ITERS = 3
MESH = pl.DeviceIdType.MESH
SUB = 8
LANE = 128
SEAM = 16


def roll(array, shift, axis):
    shift = shift % array.shape[axis]
    return pltpu.roll(array, shift, axis) if shift else array


def iota(shape, dim):
    return lax.broadcasted_iota(jnp.int32, shape, dim)


def pick(array, lanes):
    return jnp.take_along_axis(array, lanes, axis=1, mode="promise_in_bounds")


def transport(current, east, nort, open_east, open_nort):
    east = jnp.where(open_east, east, 0.0)
    nort = jnp.where(open_nort, nort, 0.0)
    for _ in range(TSTEPS):
        flux_east = east * jnp.where(east > 0.0, current, roll(current, -1, 1))
        flux_north = nort * jnp.where(nort > 0.0, current, roll(current, -1, 0))
        current = current - (flux_east - roll(flux_east, 1, 1) + flux_north - roll(flux_north, 1, 0))
    return current


def kernel(
    ny,
    nx,
    tracer_ref,
    east_ref,
    north_ref,
    columns_ref,
    thick_hbm,
    surface_ref,
    helm_ref,
    tracer_out,
    heights_out,
    fields,
    col_in,
    flat_ext,
    own_tile,
    to_east,
    to_west,
    from_west,
    from_east,
    corner,
    rows_up,
    rows_down,
    rows_south,
    rows_north,
    flat_up,
    flat_down,
    flat_south,
    flat_north,
    tile_south,
    tile_north,
    strip_south,
    strip_north,
    level_sum,
    faces,
    part,
    slots,
    thickness,
    in_sem,
    send_sem,
    recv_sem,
    sum_send_sem,
    sum_recv_sem,
):
    _, levels, rows, cols = fields.shape
    my_y, my_x = lax.axis_index("gy"), lax.axis_index("gx")
    count = ny * nx

    def wrap(value, size):
        return jnp.where(value >= size, value - size, value)

    ys = [my_y] + [wrap(my_y + d, ny) for d in range(1, ny)]
    xs = [my_x] + [wrap(my_x + d, nx) for d in range(1, nx)]
    others = [(y, x) for b, x in enumerate(xs) for a, y in enumerate(ys) if a or b]
    south_here, north_here = my_y > 0, my_y < ny - 1

    small = [
        pltpu.make_async_copy(columns_ref, col_in, in_sem.at[0]),
        pltpu.make_async_copy(helm_ref, flat_ext.at[1, 0:rows, 0:cols], in_sem.at[1]),
        pltpu.make_async_copy(surface_ref, flat_ext.at[2, 0:rows, 0:cols], in_sem.at[2]),
    ]
    large = [
        pltpu.make_async_copy(ref, fields.at[f], in_sem.at[3 + f])
        for f, ref in enumerate((tracer_ref, east_ref, north_ref))
    ]
    thick = pltpu.make_async_copy(thick_hbm, thickness, in_sem.at[6])
    for load in small + large + [thick]:
        load.start()
    barrier = pltpu.get_barrier_semaphore()
    for target in reversed(others):
        pl.semaphore_signal(barrier, inc=1, device_id=target, device_id_type=MESH)

    lane = iota((rows, LANE), 1)
    group = lane // SEAM
    seat = lane % SEAM
    first_rows, last_rows = pl.ds(0, SUB), pl.ds(rows - SUB, SUB)

    def both_edges(left, right):
        return jnp.where(lane < LANE // 2, left, right)

    def flat_edges(f):
        return both_edges(flat_ext[f, 0:rows, 0:LANE], flat_ext[f, 0:rows, cols - LANE : cols])

    def spare_lane(slot):
        return SEAM * (slot // 2) + SEAM - 2 + slot % 2

    for load in small:
        load.wait()
    flat_ext[0, 0:rows, 0:cols] = col_in[...].astype(jnp.float32)
    depth_edge = flat_edges(0)
    own_tile[3] = pick(depth_edge, (LANE - SUB + seat) % LANE)
    three = jnp.where(
        (lane < SUB) | (lane >= LANE - SUB),
        depth_edge,
        jnp.where(lane < 3 * SUB, roll(flat_edges(1), 2 * SUB, 1), roll(flat_edges(2), 4 * SUB, 1)),
    )
    slot = jnp.maximum(2 * group + seat - (SEAM - 2), 0)
    east_from = jnp.where(slot < 6, LANE - 5 + slot, jnp.where(slot < 10, slot - 6 + 13, slot - 10 + 29)) % LANE
    west_from = jnp.where(slot < 6, slot, jnp.where(slot < 10, slot - 6 + 16, slot - 10 + 32)) % LANE
    spare_east, spare_west = pick(three, east_from), pick(three, west_from)
    for f in range(3):
        flat_up[f] = flat_ext[f, rows - SUB : rows, 0:cols]
        flat_down[f] = flat_ext[f, 0:SUB, 0:cols]

    tiles = []
    for f in range(3):
        large[f].wait()
        packed = None
        for k in range(levels):
            moved = roll(both_edges(fields[f, k, :, 0:LANE], fields[f, k, :, cols - LANE : cols]), SEAM * k + SUB, 1)
            packed = moved if packed is None else jnp.where(group == k, moved, packed)
        own_tile[f] = packed
        tiles.append(packed)

    def message(shifts, spare):
        c, e, n = (roll(tile, shift, 1) for tile, shift in zip(tiles, shifts))
        return jnp.where(seat < 5, c, jnp.where(seat < 10, e, jnp.where(seat < SEAM - 2, n, spare)))

    to_east[...] = message((-3, 2, 6), spare_east)
    to_west[...] = message((-8, -3, 2), spare_west)

    sub = iota((SUB, cols), 0)
    for k in range(levels):
        c, e, n = (fields[f, k, rows - SUB : rows] for f in range(3))
        rows_up[k, 0:SUB] = jnp.where(sub < 3, roll(n, -3, 0), c)
        rows_up[k, SUB : 2 * SUB] = jnp.where(sub < 4, roll(n, 2, 0), e)
        c, e, n = (fields[f, k, 0:SUB] for f in range(3))
        rows_down[k, 0:SUB] = jnp.where(sub < 5, c, roll(n, 5, 0))
        rows_down[k, SUB : 2 * SUB] = jnp.where(sub < 4, e, roll(n, 1, 0))

    pl.semaphore_wait(barrier, count - 1)

    up, down, right, left = wrap(my_y + 1, ny), wrap(my_y + ny - 1, ny), xs[1], xs[-1]
    plan = [
        (to_east, from_west, (my_y, right)),
        (to_west, from_east, (my_y, left)),
        (rows_up, rows_south, (up, my_x)),
        (flat_up, flat_south, (up, my_x)),
        (own_tile.at[:, last_rows], tile_south, (up, my_x)),
        (to_east.at[last_rows], corner.at[0], (up, right)),
        (to_west.at[last_rows], corner.at[2], (up, left)),
        (rows_down, rows_north, (down, my_x)),
        (flat_down, flat_north, (down, my_x)),
        (own_tile.at[:, first_rows], tile_north, (down, my_x)),
        (to_east.at[first_rows], corner.at[1], (down, right)),
        (to_west.at[first_rows], corner.at[3], (down, left)),
    ]
    copies = [
        pltpu.make_async_remote_copy(
            src_ref=source,
            dst_ref=target,
            send_sem=send_sem.at[which],
            recv_sem=recv_sem.at[which],
            device_id=device,
            device_id_type=MESH,
        )
        for which, (source, target, device) in enumerate(plan)
    ]
    beside, upward, downward = copies[0:2], copies[2:7], copies[7:12]

    def each(items, act):
        for item in items:
            act(item)

    start, wait_recv, wait_send = (lambda c: c.start()), (lambda c: c.wait_recv()), (lambda c: c.wait_send())
    pl.when(north_here)(lambda: each(upward[3:], start))
    pl.when(south_here)(lambda: each(downward[3:], start))
    each(beside, start)
    pl.when(north_here)(lambda: each(upward[:3], start))
    pl.when(south_here)(lambda: each(downward[:3], start))

    thick.wait()
    depth = flat_ext[0, 0:rows, 0:cols]
    faces[0] = jnp.minimum(depth, roll(depth, -1, 1))
    faces[1] = jnp.minimum(depth, roll(depth, -1, 0))
    level_sum[0:rows, 0:cols] = jnp.zeros((rows, cols), jnp.float32)

    def level(k, carry):
        below = lax.convert_element_type(k, jnp.float32)
        current = transport(fields[0, k], fields[1, k], fields[2, k], faces[0] > below, faces[1] > below)
        tracer_out[k] = current
        open_here = flat_ext[0, 0:rows, 0:cols] > below
        level_sum[0:rows, 0:cols] += jnp.where(open_here, thickness[k] * current, 0.0)
        return carry

    lax.fori_loop(0, levels, level, 0, unroll=2)

    @pl.when(jnp.logical_not(south_here))
    def _():
        for ref in (rows_south, flat_south, tile_south):
            ref[...] = jnp.zeros(ref.shape, jnp.float32)
        for which in (0, 2):
            corner[which] = jnp.zeros((SUB, LANE), jnp.float32)

    @pl.when(jnp.logical_not(north_here))
    def _():
        for ref in (rows_north, flat_north, tile_north):
            ref[...] = jnp.zeros(ref.shape, jnp.float32)
        for which in (1, 3):
            corner[which] = jnp.zeros((SUB, LANE), jnp.float32)

    pl.when(south_here)(lambda: each(upward[:3], wait_recv))
    pl.when(north_here)(lambda: each(downward[:3], wait_recv))

    stacked_level = (iota((2 * SUB * levels, cols), 0) // (2 * SUB)).astype(jnp.float32)

    def row_strip(pieces, depth16, out):
        c, e, n = (jnp.concatenate(p, axis=0) for p in pieces)
        deep = jnp.concatenate([depth16] * levels, axis=0)
        open_east = jnp.minimum(deep, roll(deep, -1, 1)) > stacked_level
        open_nort = jnp.minimum(deep, roll(deep, -1, 0)) > stacked_level
        new = transport(c, e, n, open_east, open_nort)
        out[...] = new
        total = None
        for k in range(levels):
            term = jnp.where(depth16 > k, thickness[k] * new[2 * SUB * k : 2 * SUB * (k + 1)], 0.0)
            total = term if total is None else total + term
        return total

    south, north = ([], [], []), ([], [], [])
    for k in range(levels):
        a, b = rows_south[k, 0:SUB], rows_south[k, SUB : 2 * SUB]
        for f, halo in enumerate((a, b, jnp.where(sub < 6, roll(a, 3, 0), roll(b, -2, 0)))):
            south[f].extend([halo, fields[f, k, 0:SUB]])
        a, b = rows_north[k, 0:SUB], rows_north[k, SUB : 2 * SUB]
        for f, halo in enumerate((a, b, jnp.where(sub < 3, roll(a, -5, 0), roll(b, -1, 0)))):
            north[f].extend([fields[f, k, rows - SUB : rows], halo])
    sum_south = row_strip(south, jnp.concatenate([flat_south[0], flat_down[0]], axis=0), strip_south)
    sum_north = row_strip(north, jnp.concatenate([flat_up[0], flat_north[0]], axis=0), strip_north)
    level_sum[0:SUB, 0:cols] = jnp.where(sub < 2, sum_south[SUB:], level_sum[0:SUB, 0:cols])
    level_sum[rows - SUB : rows, 0:cols] = jnp.where(
        sub >= SUB - 2, sum_north[0:SUB], level_sum[rows - SUB : rows, 0:cols]
    )
    level_sum[rows : rows + SUB, 0:cols] = jnp.where(sub < SUB // 2, sum_north[SUB:], sum_south[0:SUB])
    for f in range(3):
        flat_ext[f, rows : rows + SUB, 0:cols] = jnp.where(sub < SUB // 2, flat_north[f], flat_south[f])

    tall = rows + 2 * SUB
    lane = iota((tall, LANE), 1)
    group = lane // SEAM
    seat = lane % SEAM
    strip_level = group.astype(jnp.float32)
    lane_thickness = jnp.zeros((tall, LANE), jnp.float32)
    for k in range(levels):
        lane_thickness = jnp.where(group == k, thickness[k], lane_thickness)
    own = [
        jnp.concatenate([tile_south[f], own_tile[f], tile_north[f]], axis=0) for f in range(4)
    ]
    low_seat = seat < SUB
    small_sub = iota((SUB, LANE), 0) < SUB // 2

    each(beside, wait_recv)
    pl.when(south_here)(lambda: each(upward[3:], wait_recv))
    pl.when(north_here)(lambda: each(downward[3:], wait_recv))

    def cyclic(array):
        turn = jnp.where(small_sub, array[rows + SUB :], array[0:SUB])
        return jnp.concatenate([array[SUB : rows + SUB], turn], axis=0)

    west = jnp.concatenate([corner[0], from_west[...], corner[1]], axis=0)
    east = jnp.concatenate([corner[2], from_east[...], corner[3]], axis=0)

    def side_strip(got, shifts, first, halo_seat):
        slots_of = jnp.minimum(jnp.maximum(seat - first, 0), 4)
        got_c, got_e, got_n = (roll(got, shift, 1) for shift in shifts)
        got_d = pick(got, spare_lane(slots_of))
        c, e, n, d = (jnp.where(halo_seat, g, o) for g, o in zip((got_c, got_e, got_n, got_d), own))
        open_east = jnp.minimum(d, roll(d, -1, 1)) > strip_level
        open_nort = jnp.minimum(d, roll(d, -1, 0)) > strip_level
        new = transport(c, e, n, open_east, open_nort)
        total = jnp.where(d > strip_level, lane_thickness * new, 0.0)
        for shift in (64, 32, 16):
            total = total + roll(total, shift, 1)
        return new, cyclic(roll(total, -SUB, 1))

    new_west, sum_west = side_strip(west, (3, -2, -6), 3, low_seat)
    new_east, sum_east = side_strip(east, (8, 3, -2), 8, jnp.logical_not(low_seat))

    flat_lane = iota((rows + SUB, LANE), 1)
    half = flat_lane < LANE // 2
    level_sum[:, cols : cols + LANE] = jnp.where(half, sum_east, sum_west)
    level_sum[:, 0:LANE] = jnp.where(flat_lane < 2, sum_west, level_sum[:, 0:LANE])
    level_sum[:, cols - LANE : cols] = jnp.where(flat_lane >= LANE - 2, sum_east, level_sum[:, cols - LANE : cols])
    for f, (base_west, base_east) in enumerate(((2, 0), (6, 6), (10, 10))):
        from_slot = jnp.where(lane < LANE // 2, base_east + (lane & 3), base_west + ((lane - (LANE - 3)) & 3))
        seen = spare_lane(from_slot)
        side = jnp.where(lane < LANE // 2, pick(east, seen), pick(west, seen))
        flat_ext[f, :, cols : cols + LANE] = cyclic(side)

    deep = flat_ext[0]
    inverse = 1.0 / (6.0 + flat_ext[1])
    wet = deep > 0.0
    scale = jnp.where(wet, inverse, 0.0)
    z0_ext = (flat_ext[2] + level_sum[...]) * inverse
    start_vec = jnp.where(wet, z0_ext, 0.0)

    def off_diagonal(vector):
        across = roll(vector, 1, 1) + roll(vector, -1, 1)
        mixed = vector + 0.5 * across
        return scale * (across + roll(mixed, 1, 0) + roll(mixed, -1, 0))

    z1_ext = off_diagonal(start_vec)
    z2_ext = off_diagonal(z1_ext)
    z3_ext = off_diagonal(z2_ext)
    z0, z1, z2, z3 = (z[0:rows, 0:cols] for z in (z0_ext, z1_ext, z2_ext, z3_ext))
    diagonal = 6.0 + flat_ext[1, 0:rows, 0:cols]

    def partial(values):
        folded = jnp.sum(values, axis=0, keepdims=True)
        return sum(folded[:, i : i + LANE] for i in range(0, cols, LANE))

    d0, d1, d2 = (diagonal * z for z in (z0, z1, z2))
    sums = [partial(v) for v in (d0 * z0, d0 * z1, d1 * z1, d1 * z2, d2 * z2, d2 * z3)]
    folded = jnp.concatenate(sums + [jnp.zeros((SUB - len(sums), LANE), jnp.float32)], axis=0)
    for shift in (64, 32, 16):
        folded = folded + roll(folded, shift, 1)
    diag = iota((SUB, LANE), 1) // (LANE // SUB) == iota((SUB, LANE), 0)
    part[...] = jnp.sum(jnp.where(diag, folded, 0.0), axis=0, keepdims=True)

    for index, target in enumerate(others):
        pltpu.make_async_remote_copy(
            src_ref=part,
            dst_ref=slots.at[index],
            send_sem=sum_send_sem,
            recv_sem=sum_recv_sem,
            device_id=target,
            device_id_type=MESH,
        ).start()

    for k in range(levels):
        tracer_out[k, 0:SUB] = jnp.where(sub < 2, strip_south[2 * SUB * k + SUB : 2 * SUB * (k + 1)], tracer_out[k, 0:SUB])
        tracer_out[k, rows - SUB : rows] = jnp.where(
            sub >= SUB - 2, strip_north[2 * SUB * k : 2 * SUB * k + SUB], tracer_out[k, rows - SUB : rows]
        )
    side_new = jnp.where(low_seat, new_east, new_west)[SUB : rows + SUB]
    lane = iota((rows, LANE), 1)
    for k in range(levels):
        moved = roll(side_new, -SEAM * k - SUB, 1)
        tracer_out[k, :, 0:LANE] = jnp.where(lane < 2, moved, tracer_out[k, :, 0:LANE])
        tracer_out[k, :, cols - LANE : cols] = jnp.where(lane >= LANE - 2, moved, tracer_out[k, :, cols - LANE : cols])

    everything = pltpu.make_async_remote_copy(
        src_ref=slots,
        dst_ref=slots,
        send_sem=sum_send_sem,
        recv_sem=sum_recv_sem,
        device_id=others[0],
        device_id_type=MESH,
    )
    everything.wait_recv()
    total = jnp.sum(slots[...], axis=0) + part[...]
    total = jnp.sum(jnp.where(diag, total, 0.0), axis=1, keepdims=True)
    moment = [total[i : i + 1, :] for i in range(2 * ITERS)]

    def inner(a, b):
        return sum(x * y * moment[i + j] for i, x in enumerate(a) for j, y in enumerate(b))

    def ratio(top, bottom):
        good = bottom > 0.0
        return jnp.where(good, top / jnp.where(good, bottom, 1.0), 0.0)

    one, zero = jnp.ones((1, 1), jnp.float32), jnp.zeros((1, 1), jnp.float32)
    scaled, direction, height = [one], [one], [zero] * ITERS
    product_now = moment[0]
    for iteration in range(ITERS):
        low, high = direction + [zero], [zero] + direction
        applied = [a - b for a, b in zip(low, high)]
        step_size = ratio(product_now, inner(direction, applied))
        for i, x in enumerate(direction):
            height[i] = height[i] + step_size * x
        if iteration + 1 < ITERS:
            scaled = [a - step_size * b for a, b in zip(scaled + [zero], applied)]
            product_next = jnp.maximum(inner(scaled, scaled), 0.0)
            factor = ratio(product_next, product_now)
            direction = [a + factor * b for a, b in zip(scaled, low)]
            product_now = product_next
    heights_out[...] = height[0] * z0 + height[1] * z1 + height[2] * z2

    everything.wait_send()
    each(beside, wait_send)
    pl.when(north_here)(lambda: each(upward, wait_send))
    pl.when(south_here)(lambda: each(downward, wait_send))


def hand_on(tracer_ref, heights_ref, tracer_out, heights_out, save):
    levels = tracer_ref.shape[0]
    stages = [(heights_ref, heights_out)]
    stages += [(tracer_ref.at[k], tracer_out.at[k]) for k in range(levels)]
    saves = [pltpu.make_async_copy(a, b, save.at[i]) for i, (a, b) in enumerate(stages)]
    for copy in saves:
        copy.start()
    for copy in saves:
        copy.wait()


def on_device(ny, nx, tracer, east_speed, north_speed, columns, thickness, surface_flux, helm):
    levels, rows, cols = tracer.shape
    ext = (rows + SUB, cols + LANE)
    hbm = pl.BlockSpec(memory_space=pl.ANY)
    vmem = pl.BlockSpec(memory_space=pltpu.VMEM)
    f32 = jnp.float32
    dma = pltpu.SemaphoreType.DMA
    scratch = [
        pltpu.VMEM((3, levels, rows, cols), f32),
        pltpu.VMEM((rows, cols), jnp.int32),
        pltpu.VMEM((3, *ext), f32),
        pltpu.VMEM((4, rows, LANE), f32),
        *[pltpu.VMEM((rows, LANE), f32)] * 4,
        pltpu.VMEM((4, SUB, LANE), f32),
        *[pltpu.VMEM((levels, 2 * SUB, cols), f32)] * 4,
        *[pltpu.VMEM((3, SUB, cols), f32)] * 4,
        *[pltpu.VMEM((4, SUB, LANE), f32)] * 2,
        *[pltpu.VMEM((levels * 2 * SUB, cols), f32)] * 2,
        pltpu.VMEM(ext, f32),
        pltpu.VMEM((2, rows, cols), f32),
        pltpu.VMEM((1, LANE), f32),
        pltpu.VMEM((ny * nx - 1, 1, LANE), f32),
        pltpu.SMEM((levels,), f32),
        dma((7,)),
        dma((12,)),
        dma((12,)),
        dma,
        dma,
    ]
    results = pl.pallas_call(
        functools.partial(kernel, ny, nx),
        out_shape=(
            pltpu.VMEM((levels, rows, cols), f32),
            pltpu.VMEM((rows, cols), f32),
        ),
        in_specs=[hbm] * 7,
        out_specs=(vmem, vmem),
        scratch_shapes=scratch,
        compiler_params=pltpu.CompilerParams(collective_id=0, has_side_effects=True),
    )(tracer, east_speed, north_speed, columns, thickness, surface_flux, helm)
    return pl.pallas_call(
        hand_on,
        out_shape=tuple(jax.ShapeDtypeStruct(r.shape, f32) for r in results),
        in_specs=[vmem, vmem],
        out_specs=(hbm, hbm),
        scratch_shapes=[dma((levels + 1,))],
    )(*[pltpu.with_memory_space_constraint(r, pltpu.VMEM) for r in results])


def solution(mesh):
    spec = P(None, "gy", "gx")
    flat = P("gy", "gx")
    return jax.shard_map(
        functools.partial(on_device, mesh.shape["gy"], mesh.shape["gx"]),
        mesh=mesh,
        in_specs=(spec, spec, spec, flat, P(), flat, flat),
        out_specs=(spec, flat),
        check_vma=False,
    )
```

```python
import functools

import jax
import jax.numpy as jnp
from jax import lax
from jax.experimental import pallas as pl
from jax.experimental.pallas import tpu as pltpu
from jax.sharding import PartitionSpec as P

TSTEPS = 2
ITERS = 3
MESH = pl.DeviceIdType.MESH
SUB = 8
LANE = 128
SEAM = 16


def roll(array, shift, axis):
    shift = shift % array.shape[axis]
    return pltpu.roll(array, shift, axis) if shift else array


def iota(shape, dim):
    return lax.broadcasted_iota(jnp.int32, shape, dim)


def pick(array, lanes):
    return jnp.take_along_axis(array, lanes, axis=1, mode="promise_in_bounds")


def transport(current, east, nort, open_east, open_nort):
    east = jnp.where(open_east, east, 0.0)
    nort = jnp.where(open_nort, nort, 0.0)
    for _ in range(TSTEPS):
        flux_east = east * jnp.where(east > 0.0, current, roll(current, -1, 1))
        flux_north = nort * jnp.where(nort > 0.0, current, roll(current, -1, 0))
        current = current - (flux_east - roll(flux_east, 1, 1) + flux_north - roll(flux_north, 1, 0))
    return current


def kernel(
    ny,
    nx,
    tracer_ref,
    east_ref,
    north_ref,
    columns_ref,
    thick_hbm,
    surface_ref,
    helm_ref,
    tracer_out,
    basis_out,
    moments_out,
    fields,
    col_in,
    flat,
    own_tile,
    to_east,
    to_west,
    west,
    east,
    rows_up,
    rows_down,
    rows_south,
    rows_north,
    strip_south,
    strip_north,
    own_sum,
    faces,
    strips,
    level_sum,
    scale,
    start_vec,
    part,
    slots,
    thickness,
    know_sem,
    in_sem,
    send_sem,
    recv_sem,
    sum_send_sem,
    sum_recv_sem,
):
    _, levels, rows, cols = fields.shape
    my_y, my_x = lax.axis_index("gy"), lax.axis_index("gx")

    def wrap(value, size):
        return jnp.where(value >= size, value - size, value)

    ys = [my_y] + [wrap(my_y + d, ny) for d in range(1, ny)]
    xs = [my_x] + [wrap(my_x + d, nx) for d in range(1, nx)]
    others = [(y, x) for b, x in enumerate(xs) for a, y in enumerate(ys) if a or b]
    south_here, north_here = my_y > 0, my_y < ny - 1

    blocks = range(cols // LANE)
    side_block = cols // LANE
    inside = pl.ds(SUB, rows)
    small = [pltpu.make_async_copy(columns_ref, col_in, in_sem.at[0])] + [
        pltpu.make_async_copy(ref.at[:, pl.ds(LANE * b, LANE)], flat.at[f, b, inside], in_sem.at[7 + len(blocks) * (f - 1) + b])
        for f, ref in ((1, helm_ref), (2, surface_ref))
        for b in blocks
    ]
    large = [
        pltpu.make_async_copy(ref, fields.at[f], in_sem.at[3 + f])
        for f, ref in enumerate((tracer_ref, east_ref, north_ref))
    ]
    thick = pltpu.make_async_copy(thick_hbm, thickness, in_sem.at[6])
    for load in small + large + [thick]:
        load.start()
    barrier = pltpu.get_barrier_semaphore()

    def around(reach_y, reach_x):
        return [(ys[a], xs[b]) for a in reach_y for b in reach_x if a or b]

    def reach(distance, known, size):
        return (0,) if 2 * known + 1 >= size else (distance, -distance, 0)

    greeted = around(reach(1, 0, ny), reach(1, 0, nx))
    for target in greeted:
        pl.semaphore_signal(barrier, inc=1, device_id=target, device_id_type=MESH)
    rounds, known = [], 1
    while 2 * known + 1 < max(ny, nx):
        rounds.append(around(reach(known, known, ny), reach(known, known, nx)))
        known *= 2

    def tell(turn):
        for target in rounds[turn]:
            pl.semaphore_signal(know_sem.at[turn], inc=1, device_id=target, device_id_type=MESH)

    def hear(turn):
        pl.semaphore_wait(know_sem.at[turn], len(rounds[turn]))


    lane = iota((rows, LANE), 1)
    group = lane // SEAM
    seat = lane % SEAM
    first_rows, last_rows = pl.ds(0, SUB), pl.ds(rows - SUB, SUB)
    low_halo, low_own, high_own, high_halo = (pl.ds(at, SUB) for at in (0, SUB, rows, rows + SUB))

    def both_edges(left, right):
        return jnp.where(lane < LANE // 2, left, right)

    def flat_edges(f):
        return both_edges(flat[f, 0, inside], flat[f, side_block - 1, inside])

    def spare_lane(slot):
        return SEAM * (slot // 2) + SEAM - 2 + slot % 2

    for load in small:
        load.wait()
    for b in blocks:
        flat[0, b, inside] = col_in[:, LANE * b : LANE * (b + 1)].astype(jnp.float32)
    depth_edge = flat_edges(0)
    own_tile[3, inside] = pick(depth_edge, (LANE - SUB + seat) % LANE)
    three = jnp.where(
        (lane < SUB) | (lane >= LANE - SUB),
        depth_edge,
        jnp.where(lane < 3 * SUB, roll(flat_edges(1), 2 * SUB, 1), roll(flat_edges(2), 4 * SUB, 1)),
    )
    slot = jnp.maximum(2 * group + seat - (SEAM - 2), 0)
    east_from = jnp.where(slot < 6, LANE - 5 + slot, jnp.where(slot < 10, slot - 6 + 13, slot - 10 + 29)) % LANE
    west_from = jnp.where(slot < 6, slot, jnp.where(slot < 10, slot - 6 + 16, slot - 10 + 32)) % LANE
    spare_east, spare_west = pick(three, east_from), pick(three, west_from)
    tiles = []
    for f in range(3):
        large[f].wait()
        packed = None
        for k in range(levels):
            moved = roll(both_edges(fields[f, k, :, 0:LANE], fields[f, k, :, cols - LANE : cols]), SEAM * k + SUB, 1)
            packed = moved if packed is None else jnp.where(group == k, moved, packed)
        own_tile[f, inside] = packed
        tiles.append(packed)

    def message(shifts, spare):
        c, e, n = (roll(tile, shift, 1) for tile, shift in zip(tiles, shifts))
        return jnp.where(seat < 5, c, jnp.where(seat < 10, e, jnp.where(seat < SEAM - 2, n, spare)))

    to_east[...] = message((-3, 2, 6), spare_east)
    to_west[...] = message((-8, -3, 2), spare_west)

    sub = iota((SUB, cols), 0)
    for k in range(levels):
        c, e, n = (fields[f, k, rows - SUB : rows] for f in range(3))
        rows_up[k, 0:SUB] = jnp.where(sub < 3, roll(n, -3, 0), c)
        rows_up[k, SUB : 2 * SUB] = jnp.where(sub < 4, roll(n, 2, 0), e)
        c, e, n = (fields[f, k, 0:SUB] for f in range(3))
        rows_down[k, 0:SUB] = jnp.where(sub < 5, c, roll(n, 5, 0))
        rows_down[k, SUB : 2 * SUB] = jnp.where(sub < 4, e, roll(n, 1, 0))

    pl.semaphore_wait(barrier, len(greeted))

    up, down, right, left = wrap(my_y + 1, ny), wrap(my_y + ny - 1, ny), xs[1], xs[-1]
    body = pl.ds(0, side_block)
    plan = [
        (to_east, west.at[inside], (my_y, right)),
        (to_west, east.at[inside], (my_y, left)),
        (rows_up, rows_south, (up, my_x)),
        (flat.at[:, body, high_own], flat.at[:, body, low_halo], (up, my_x)),
        (own_tile.at[:, high_own], own_tile.at[:, low_halo], (up, my_x)),
        (to_east.at[last_rows], west.at[low_halo], (up, right)),
        (to_west.at[last_rows], east.at[low_halo], (up, left)),
        (rows_down, rows_north, (down, my_x)),
        (flat.at[:, body, low_own], flat.at[:, body, high_halo], (down, my_x)),
        (own_tile.at[:, low_own], own_tile.at[:, high_halo], (down, my_x)),
        (to_east.at[first_rows], west.at[high_halo], (down, right)),
        (to_west.at[first_rows], east.at[high_halo], (down, left)),
    ]
    copies = [
        pltpu.make_async_remote_copy(
            src_ref=source,
            dst_ref=target,
            send_sem=send_sem.at[which],
            recv_sem=recv_sem.at[which],
            device_id=device,
            device_id_type=MESH,
        )
        for which, (source, target, device) in enumerate(plan)
    ]
    beside, upward, downward = copies[0:2], copies[2:7], copies[7:12]

    def each(items, act):
        for item in items:
            act(item)

    start, wait_recv, wait_send = (lambda c: c.start()), (lambda c: c.wait_recv()), (lambda c: c.wait_send())
    pl.when(north_here)(lambda: each(upward[3:], start))
    pl.when(south_here)(lambda: each(downward[3:], start))
    each(beside, start)
    pl.when(north_here)(lambda: each(upward[:3], start))
    pl.when(south_here)(lambda: each(downward[:3], start))
    if rounds:
        tell(0)

    thick.wait()
    depth = col_in[...].astype(jnp.float32)
    faces[0] = jnp.minimum(depth, roll(depth, -1, 1))
    faces[1] = jnp.minimum(depth, roll(depth, -1, 0))
    own_sum[...] = jnp.zeros((rows, cols), jnp.float32)

    def level(k, carry):
        below = lax.convert_element_type(k, jnp.float32)
        current = transport(fields[0, k], fields[1, k], fields[2, k], faces[0] > below, faces[1] > below)
        tracer_out[k] = current
        own_sum[...] += jnp.where(col_in[...] > k, thickness[k] * current, 0.0)
        return carry

    lax.fori_loop(0, levels, level, 0, unroll=2)

    def blank(rows_ref, halo):
        rows_ref[...] = jnp.zeros(rows_ref.shape, jnp.float32)
        flat[:, body, halo] = jnp.zeros((3, side_block, SUB, LANE), jnp.float32)
        own_tile[:, halo] = jnp.zeros((4, SUB, LANE), jnp.float32)
        for ref in (west, east):
            ref[halo] = jnp.zeros((SUB, LANE), jnp.float32)

    pl.when(jnp.logical_not(south_here))(lambda: blank(rows_south, low_halo))
    pl.when(jnp.logical_not(north_here))(lambda: blank(rows_north, high_halo))

    for turn in range(1, len(rounds)):
        hear(turn - 1)
        tell(turn)
    pl.when(south_here)(lambda: each(upward[:3], wait_recv))
    pl.when(north_here)(lambda: each(downward[:3], wait_recv))

    stacked_level = (iota((2 * SUB * levels, cols), 0) // (2 * SUB)).astype(jnp.float32)

    def row_strip(pieces, depth16, out):
        c, e, n = (jnp.concatenate(p, axis=0) for p in pieces)
        deep = jnp.concatenate([depth16] * levels, axis=0)
        open_east = jnp.minimum(deep, roll(deep, -1, 1)) > stacked_level
        open_nort = jnp.minimum(deep, roll(deep, -1, 0)) > stacked_level
        new = transport(c, e, n, open_east, open_nort)
        out[...] = new
        total = None
        for k in range(levels):
            term = jnp.where(depth16 > k, thickness[k] * new[2 * SUB * k : 2 * SUB * (k + 1)], 0.0)
            total = term if total is None else total + term
        return total

    south, north = ([], [], []), ([], [], [])
    for k in range(levels):
        a, b = rows_south[k, 0:SUB], rows_south[k, SUB : 2 * SUB]
        for f, halo in enumerate((a, b, jnp.where(sub < 6, roll(a, 3, 0), roll(b, -2, 0)))):
            south[f].extend([halo, fields[f, k, 0:SUB]])
        a, b = rows_north[k, 0:SUB], rows_north[k, SUB : 2 * SUB]
        for f, halo in enumerate((a, b, jnp.where(sub < 3, roll(a, -5, 0), roll(b, -1, 0)))):
            north[f].extend([fields[f, k, rows - SUB : rows], halo])
    def depth_rows(at):
        return jnp.concatenate([flat[0, b, at : at + 2 * SUB] for b in blocks], axis=1)

    sum_south = row_strip(south, depth_rows(0), strip_south)
    sum_north = row_strip(north, depth_rows(rows), strip_north)
    for b in blocks:
        here = slice(LANE * b, LANE * (b + 1))
        level_sum[b, 0:SUB] = sum_south[0:SUB, here]
        level_sum[b, inside] = own_sum[:, here]
        level_sum[b, SUB : SUB + 2] = sum_south[SUB : SUB + 2, here]
        level_sum[b, rows + SUB - 2 : rows + SUB] = sum_north[SUB - 2 : SUB, here]
        level_sum[b, rows + SUB : rows + 2 * SUB] = sum_north[SUB:, here]
        scale[b, 0 : rows + 2 * SUB] = 1.0 / (6.0 + flat[1, b])

    lane = iota((SUB, LANE), 1)
    group = lane // SEAM
    seat = lane % SEAM
    strip_level = group.astype(jnp.float32)
    lane_thickness = jnp.zeros((SUB, LANE), jnp.float32)
    for k in range(levels):
        lane_thickness = jnp.where(group == k, thickness[k], lane_thickness)
    low_half = lane < LANE // 2

    def side_lanes(base_west, base_east):
        return spare_lane(jnp.where(low_half, base_east + (lane & 3), base_west + ((lane - (LANE - 3)) & 3)))

    side_pick = [side_lanes(*bases) for bases in ((2, 0), (6, 6), (10, 10))]
    sides = []
    for got, shifts, first, in_halo in (
        (west, (3, -2, -6), 3, seat < SUB),
        (east, (8, 3, -2), 8, seat >= SUB),
    ):
        depth_pick = spare_lane(jnp.minimum(jnp.maximum(seat - first, 0), 4))
        sides.append((got, shifts, depth_pick, in_halo))

    each(beside, wait_recv)
    pl.when(south_here)(lambda: each(upward[3:], wait_recv))
    pl.when(north_here)(lambda: each(downward[3:], wait_recv))

    def at(start):
        return slice(start, start + SUB)

    for r in range(0, rows + 2 * SUB, SUB):
        for w, (got, shifts, depth_pick, in_halo) in enumerate(sides):
            sent = got[at(r)]
            moved = [roll(sent, shift, 1) for shift in shifts] + [pick(sent, depth_pick)]
            for f in range(4):
                strips[w, f, at(r)] = jnp.where(in_halo, moved[f], own_tile[f, at(r)])
    for r in range(0, rows + 2 * SUB, SUB):
        for w in range(2):
            deep = strips[w, 3, at(r)]
            open_east = jnp.minimum(deep, roll(deep, -1, 1)) > strip_level
            open_nort = jnp.minimum(deep, strips[w, 3, at(r + 1)]) > strip_level
            strips[w, 1, at(r)] = jnp.where(open_east, strips[w, 1, at(r)], 0.0)
            strips[w, 2, at(r)] = jnp.where(open_nort, strips[w, 2, at(r)], 0.0)

    def side_step(w, f, r):
        here, ahead, behind = (strips[w, f, at(r + d)] for d in (0, 1, -1))
        fast_east, fast_north, fast_south = strips[w, 1, at(r)], strips[w, 2, at(r)], strips[w, 2, at(r - 1)]
        flux_east = fast_east * jnp.where(fast_east > 0.0, here, roll(here, -1, 1))
        flux_north = fast_north * jnp.where(fast_north > 0.0, here, ahead)
        flux_south = fast_south * jnp.where(fast_south > 0.0, behind, here)
        return here - (flux_east - roll(flux_east, 1, 1) + flux_north - flux_south)

    for r in range(SUB - 4, rows + SUB + 4, SUB):
        for w in range(2):
            strips[w, 4, at(r)] = side_step(w, 0, r)
    inner_rows = range(SUB - 3, rows + SUB + 3, SUB)
    for r in inner_rows:
        for w in range(2):
            new = side_step(w, 4, r)
            strips[w, 5, at(r)] = new
            strips[w, 0, at(r)] = jnp.where(strips[w, 3, at(r)] > strip_level, lane_thickness * new, 0.0)
    for f, lanes in enumerate(side_pick):
        for r in range(0, rows + 2 * SUB, SUB):
            flat[f, side_block, at(r)] = jnp.where(low_half, pick(east[at(r)], lanes), pick(west[at(r)], lanes))
    for r in inner_rows:
        for w in range(2):
            total = strips[w, 0, at(r)]
            strips[w, 1, at(r)] = total + roll(total, LANE // 2, 1)
    for r in inner_rows:
        for w in range(2):
            total = strips[w, 1, at(r)]
            strips[w, 2, at(r)] = sum(roll(total, shift - SUB, 1) for shift in range(0, LANE // 2, SEAM))
    for r in inner_rows:
        sum_west, sum_east = strips[0, 2, at(r)], strips[1, 2, at(r)]
        for b in range(side_block + 1):
            if b < side_block:
                total, inverse = level_sum[b, at(r)], scale[b, at(r)]
                if b == 0:
                    total = jnp.where(lane < 2, sum_west, total)
                if b == side_block - 1:
                    total = jnp.where(lane >= LANE - 2, sum_east, total)
            else:
                total = jnp.where(low_half, sum_east, sum_west)
                inverse = 1.0 / (6.0 + flat[1, b, at(r)])
            z0 = (flat[2, b, at(r)] + total) * inverse
            if b < side_block:
                level_sum[b, at(r)] = z0
            wet = flat[0, b, at(r)] > 0.0
            scale[b, at(r)] = jnp.where(wet, inverse, 0.0)
            start_vec[0, b, at(r)] = jnp.where(wet, z0, 0.0)

    def off_diagonal(source, r, wanted):
        upright, mixed = [], []
        for b in range(side_block + 1):
            both = start_vec[source, b, at(r - 1)] + start_vec[source, b, at(r + 1)]
            upright.append(both)
            mixed.append(start_vec[source, b, at(r)] + 0.5 * both)
        ahead, behind = ([roll(m, d, 1) for m in mixed] for d in (-1, 1))
        out = []
        for b in range(wanted):
            after = jnp.where(lane < LANE - 1, ahead[b], ahead[(b + 1) % (side_block + 1)])
            before = jnp.where(lane > 0, behind[b], behind[b - 1])
            out.append(scale[b, at(r)] * (upright[b] + after + before))
        return out

    for power in (1, 2):
        for r in range(SUB - 3 + power, rows + SUB + 3 - power, SUB):
            for b, z in enumerate(off_diagonal(power - 1, r, side_block + 1)):
                start_vec[power, b, at(r)] = z

    sums = [jnp.zeros((SUB, LANE), jnp.float32)] * (2 * ITERS)
    for r in range(SUB, rows + SUB, SUB):
        for b, z3 in enumerate(off_diagonal(2, r, side_block)):
            z = [level_sum[b, at(r)], start_vec[1, b, at(r)], start_vec[2, b, at(r)], z3]
            for i in range(ITERS):
                basis_out[i, b, at(r - SUB)] = z[i]
                scaled = (6.0 + flat[1, b, at(r)]) * z[i]
                sums[2 * i] += scaled * z[i]
                sums[2 * i + 1] += scaled * z[i + 1]
    sums = [jnp.sum(total, axis=0, keepdims=True) for total in sums]
    folded = jnp.concatenate(sums + [jnp.zeros((SUB - len(sums), LANE), jnp.float32)], axis=0)
    diag = iota((SUB, LANE), 1) == iota((SUB, LANE), 0)
    folded = jnp.sum(folded, axis=1, keepdims=True)
    part[...] = jnp.sum(jnp.where(diag, folded, 0.0), axis=0, keepdims=True)

    if rounds:
        hear(len(rounds) - 1)
    for index, target in enumerate(others):
        pltpu.make_async_remote_copy(
            src_ref=part,
            dst_ref=slots.at[index],
            send_sem=sum_send_sem,
            recv_sem=sum_recv_sem,
            device_id=target,
            device_id_type=MESH,
        ).start()

    for k in range(levels):
        tracer_out[k, 0:SUB] = jnp.where(sub < 2, strip_south[2 * SUB * k + SUB : 2 * SUB * (k + 1)], tracer_out[k, 0:SUB])
        tracer_out[k, rows - SUB : rows] = jnp.where(
            sub >= SUB - 2, strip_north[2 * SUB * k : 2 * SUB * k + SUB], tracer_out[k, rows - SUB : rows]
        )
    lane = iota((rows, LANE), 1)
    side_new = jnp.where(lane % SEAM < SUB, strips[1, 5, inside], strips[0, 5, inside])
    for k in range(levels):
        moved = roll(side_new, -SEAM * k - SUB, 1)
        tracer_out[k, :, 0:LANE] = jnp.where(lane < 2, moved, tracer_out[k, :, 0:LANE])
        tracer_out[k, :, cols - LANE : cols] = jnp.where(lane >= LANE - 2, moved, tracer_out[k, :, cols - LANE : cols])

    everything = pltpu.make_async_remote_copy(
        src_ref=slots,
        dst_ref=slots,
        send_sem=sum_send_sem,
        recv_sem=sum_recv_sem,
        device_id=others[0],
        device_id_type=MESH,
    )
    everything.wait_recv()
    moments_out[...] = jnp.sum(slots[...], axis=0) + part[...]

    everything.wait_send()
    each(beside, wait_send)
    pl.when(north_here)(lambda: each(upward, wait_send))
    pl.when(south_here)(lambda: each(downward, wait_send))


def finish(tracer_ref, basis_ref, moments_ref, tracer_out, heights_out, heights, save):
    levels = tracer_ref.shape[0]
    saves = [pltpu.make_async_copy(tracer_ref.at[k], tracer_out.at[k], save.at[k]) for k in range(levels)]
    for copy in saves:
        copy.start()
    diag = iota((SUB, LANE), 1) == iota((SUB, LANE), 0)
    total = jnp.broadcast_to(moments_ref[...], (SUB, LANE))
    total = jnp.sum(jnp.where(diag, total, 0.0), axis=1, keepdims=True)
    moment = [total[i : i + 1, :] for i in range(2 * ITERS)]

    def inner(a, b):
        return sum(x * y * moment[i + j] for i, x in enumerate(a) for j, y in enumerate(b))

    def ratio(top, bottom):
        good = bottom > 0.0
        return jnp.where(good, top / jnp.where(good, bottom, 1.0), 0.0)

    one, zero = jnp.ones((1, 1), jnp.float32), jnp.zeros((1, 1), jnp.float32)
    scaled, direction, height = [one], [one], [zero] * ITERS
    product_now = moment[0]
    for iteration in range(ITERS):
        low, high = direction + [zero], [zero] + direction
        applied = [a - b for a, b in zip(low, high)]
        step_size = ratio(product_now, inner(direction, applied))
        for i, x in enumerate(direction):
            height[i] = height[i] + step_size * x
        if iteration + 1 < ITERS:
            scaled = [a - step_size * b for a, b in zip(scaled + [zero], applied)]
            product_next = jnp.maximum(inner(scaled, scaled), 0.0)
            factor = ratio(product_next, product_now)
            direction = [a + factor * b for a, b in zip(scaled, low)]
            product_now = product_next
    for b in range(basis_ref.shape[1]):
        heights[:, LANE * b : LANE * (b + 1)] = sum(h * basis_ref[i, b] for i, h in enumerate(height))

    saves.append(pltpu.make_async_copy(heights, heights_out, save.at[levels]))
    saves[-1].start()
    for copy in saves:
        copy.wait()


def on_device(ny, nx, tracer, east_speed, north_speed, columns, thickness, surface_flux, helm):
    levels, rows, cols = tracer.shape
    hbm = pl.BlockSpec(memory_space=pl.ANY)
    vmem = pl.BlockSpec(memory_space=pltpu.VMEM)
    f32 = jnp.float32
    dma = pltpu.SemaphoreType.DMA
    blocks = cols // LANE
    tall = rows + 2 * SUB
    scratch = [
        pltpu.VMEM((3, levels, rows, cols), f32),
        pltpu.VMEM((rows, cols), jnp.int32),
        pltpu.VMEM((3, blocks + 1, tall, LANE), f32),
        pltpu.VMEM((4, tall, LANE), f32),
        *[pltpu.VMEM((rows, LANE), f32)] * 2,
        *[pltpu.VMEM((tall, LANE), f32)] * 2,
        *[pltpu.VMEM((levels, 2 * SUB, cols), f32)] * 4,
        *[pltpu.VMEM((levels * 2 * SUB, cols), f32)] * 2,
        pltpu.VMEM((rows, cols), f32),
        pltpu.VMEM((2, rows, cols), f32),
        pltpu.VMEM((2, 6, tall + SUB, LANE), f32),
        pltpu.VMEM((blocks + 1, tall, LANE), f32),
        pltpu.VMEM((blocks + 1, tall, LANE), f32),
        pltpu.VMEM((ITERS, blocks + 1, tall + SUB, LANE), f32),
        pltpu.VMEM((1, LANE), f32),
        pltpu.VMEM((ny * nx - 1, 1, LANE), f32),
        pltpu.SMEM((levels,), f32),
        pltpu.SemaphoreType.REGULAR((max(ny, nx).bit_length(),)),
        dma((7 + 2 * blocks,)),
        dma((12,)),
        dma((12,)),
        dma,
        dma,
    ]
    results = pl.pallas_call(
        functools.partial(kernel, ny, nx),
        out_shape=(
            pltpu.VMEM((levels, rows, cols), f32),
            pltpu.VMEM((ITERS, blocks, rows, LANE), f32),
            pltpu.VMEM((1, LANE), f32),
        ),
        in_specs=[hbm] * 7,
        out_specs=(vmem,) * 3,
        scratch_shapes=scratch,
        compiler_params=pltpu.CompilerParams(collective_id=0, has_side_effects=True),
    )(tracer, east_speed, north_speed, columns, thickness, surface_flux, helm)
    return pl.pallas_call(
        finish,
        out_shape=(
            jax.ShapeDtypeStruct((levels, rows, cols), f32),
            jax.ShapeDtypeStruct((rows, cols), f32),
        ),
        in_specs=[vmem] * 3,
        out_specs=(hbm, hbm),
        scratch_shapes=[pltpu.VMEM((rows, cols), f32), dma((levels + 1,))],
    )(*[pltpu.with_memory_space_constraint(r, pltpu.VMEM) for r in results])


def solution(mesh):
    spec = P(None, "gy", "gx")
    flat = P("gy", "gx")
    return jax.shard_map(
        functools.partial(on_device, mesh.shape["gy"], mesh.shape["gx"]),
        mesh=mesh,
        in_specs=(spec, spec, spec, flat, P(), flat, flat),
        out_specs=(spec, flat),
        check_vma=False,
    )
```

```python
import functools

import jax
import jax.numpy as jnp
from jax import lax
from jax.experimental import pallas as pl
from jax.experimental.pallas import tpu as pltpu
from jax.sharding import PartitionSpec as P

TSTEPS = 2
ITERS = 3
MESH = pl.DeviceIdType.MESH
SUB = 8
LANE = 128
SEAM = 16


def roll(array, shift, axis):
    shift = shift % array.shape[axis]
    return pltpu.roll(array, shift, axis) if shift else array


def iota(shape, dim):
    return lax.broadcasted_iota(jnp.int32, shape, dim)


def pick(array, lanes):
    return jnp.take_along_axis(array, lanes, axis=1, mode="promise_in_bounds")


def transport(current, east, nort, open_east, open_nort):
    east = jnp.where(open_east, east, 0.0)
    nort = jnp.where(open_nort, nort, 0.0)
    for _ in range(TSTEPS):
        flux_east = east * jnp.where(east > 0.0, current, roll(current, -1, 1))
        flux_north = nort * jnp.where(nort > 0.0, current, roll(current, -1, 0))
        current = current - (flux_east - roll(flux_east, 1, 1) + flux_north - roll(flux_north, 1, 0))
    return current


def kernel(
    ny,
    nx,
    tracer_ref,
    east_ref,
    north_ref,
    columns_ref,
    thick_hbm,
    surface_ref,
    helm_ref,
    tracer_out,
    basis_out,
    moments_out,
    fields,
    col_in,
    flat,
    own_tile,
    to_east,
    to_west,
    west,
    east,
    rows_up,
    rows_down,
    rows_south,
    rows_north,
    row_strips,
    own_sum,
    faces,
    strips,
    level_sum,
    scale,
    start_vec,
    part,
    slots,
    thickness,
    know_sem,
    in_sem,
    send_sem,
    recv_sem,
    sum_send_sem,
    sum_recv_sem,
):
    _, levels, rows, cols = fields.shape
    my_y, my_x = lax.axis_index("gy"), lax.axis_index("gx")

    def wrap(value, size):
        return jnp.where(value >= size, value - size, value)

    ys = [my_y] + [wrap(my_y + d, ny) for d in range(1, ny)]
    xs = [my_x] + [wrap(my_x + d, nx) for d in range(1, nx)]
    others = [(y, x) for b, x in enumerate(xs) for a, y in enumerate(ys) if a or b]
    south_here, north_here = my_y > 0, my_y < ny - 1

    blocks = range(cols // LANE)
    side_block = cols // LANE
    inside = pl.ds(SUB, rows)
    small = [pltpu.make_async_copy(columns_ref, col_in, in_sem.at[0])] + [
        pltpu.make_async_copy(ref.at[:, pl.ds(LANE * b, LANE)], flat.at[f, b, inside], in_sem.at[7 + len(blocks) * (f - 1) + b])
        for f, ref in ((1, helm_ref), (2, surface_ref))
        for b in blocks
    ]
    large = [
        pltpu.make_async_copy(ref, fields.at[f], in_sem.at[3 + f])
        for f, ref in enumerate((tracer_ref, east_ref, north_ref))
    ]
    thick = pltpu.make_async_copy(thick_hbm, thickness, in_sem.at[6])
    for load in small + large + [thick]:
        load.start()
    barrier = pltpu.get_barrier_semaphore()

    def around(reach_y, reach_x):
        return [(ys[a], xs[b]) for a in reach_y for b in reach_x if a or b]

    def reach(distance, known, size):
        return (0,) if 2 * known + 1 >= size else (distance, -distance, 0)

    greeted = around(reach(1, 0, ny), reach(1, 0, nx))
    for target in greeted:
        pl.semaphore_signal(barrier, inc=1, device_id=target, device_id_type=MESH)
    rounds, known = [], 1
    while 2 * known + 1 < max(ny, nx):
        rounds.append(around(reach(known, known, ny), reach(known, known, nx)))
        known *= 2

    def tell(turn):
        for target in rounds[turn]:
            pl.semaphore_signal(know_sem.at[turn], inc=1, device_id=target, device_id_type=MESH)

    def hear(turn):
        pl.semaphore_wait(know_sem.at[turn], len(rounds[turn]))


    lane = iota((rows, LANE), 1)
    group = lane // SEAM
    seat = lane % SEAM
    first_rows, last_rows = pl.ds(0, SUB), pl.ds(rows - SUB, SUB)
    low_halo, low_own, high_own, high_halo = (pl.ds(at, SUB) for at in (0, SUB, rows, rows + SUB))

    def both_edges(left, right):
        return jnp.where(lane < LANE // 2, left, right)

    def flat_edges(f):
        return both_edges(flat[f, 0, inside], flat[f, side_block - 1, inside])

    def spare_lane(slot):
        return SEAM * (slot // 2) + SEAM - 2 + slot % 2

    for load in small:
        load.wait()
    for b in blocks:
        flat[0, b, inside] = col_in[:, LANE * b : LANE * (b + 1)].astype(jnp.float32)
    depth_edge = flat_edges(0)
    own_tile[3, inside] = pick(depth_edge, (LANE - SUB + seat) % LANE)
    three = jnp.where(
        (lane < SUB) | (lane >= LANE - SUB),
        depth_edge,
        jnp.where(lane < 3 * SUB, roll(flat_edges(1), 2 * SUB, 1), roll(flat_edges(2), 4 * SUB, 1)),
    )
    slot = jnp.maximum(2 * group + seat - (SEAM - 2), 0)
    east_from = jnp.where(slot < 6, LANE - 5 + slot, jnp.where(slot < 10, slot - 6 + 13, slot - 10 + 29)) % LANE
    west_from = jnp.where(slot < 6, slot, jnp.where(slot < 10, slot - 6 + 16, slot - 10 + 32)) % LANE
    spare_east, spare_west = pick(three, east_from), pick(three, west_from)
    tiles = []
    for f in range(3):
        large[f].wait()
        packed = None
        for k in range(levels):
            moved = roll(both_edges(fields[f, k, :, 0:LANE], fields[f, k, :, cols - LANE : cols]), SEAM * k + SUB, 1)
            packed = moved if packed is None else jnp.where(group == k, moved, packed)
        own_tile[f, inside] = packed
        tiles.append(packed)

    def message(shifts, spare):
        c, e, n = (roll(tile, shift, 1) for tile, shift in zip(tiles, shifts))
        return jnp.where(seat < 5, c, jnp.where(seat < 10, e, jnp.where(seat < SEAM - 2, n, spare)))

    to_east[...] = message((-3, 2, 6), spare_east)
    to_west[...] = message((-8, -3, 2), spare_west)

    sub = iota((SUB, LANE), 0)
    spare_up = ((0, -1), (0, -3), (0, -5), (1, -3), (1, -5), (2, -3), (2, -5))
    spare_down = ((0, 5), (0, 2), (1, 5), (2, 5))

    def spare_rows(which, k, b, where):
        field, turn = which[min(k, len(which) - 1)]
        return roll(flat[field, b, where], turn, 0)

    for k in range(levels):
        for b in blocks:
            here = slice(LANE * b, LANE * (b + 1))
            c, e, n = (fields[f, k, rows - SUB : rows, here] for f in range(3))
            rows_up[k, b, 0:SUB] = jnp.where(sub < 3, roll(n, -3, 0), c)
            rows_up[k, b, SUB : 2 * SUB] = jnp.where(
                sub < 2, roll(n, 2, 0), jnp.where(sub < 4, spare_rows(spare_up, k, b, high_own), e)
            )
            c, e, n = (fields[f, k, 0:SUB, here] for f in range(3))
            rows_down[k, b, 0:SUB] = jnp.where(sub < 5, c, roll(n, 5, 0))
            rows_down[k, b, SUB : 2 * SUB] = jnp.where(
                sub < 4, e, jnp.where(sub < 5, roll(n, 1, 0), spare_rows(spare_down, k, b, low_own))
            )

    pl.semaphore_wait(barrier, len(greeted))

    up, down, right, left = wrap(my_y + 1, ny), wrap(my_y + ny - 1, ny), xs[1], xs[-1]
    plan = [
        (to_east, west.at[inside], (my_y, right)),
        (to_west, east.at[inside], (my_y, left)),
        (rows_up, rows_south, (up, my_x)),
        (to_east.at[last_rows], west.at[low_halo], (up, right)),
        (to_west.at[last_rows], east.at[low_halo], (up, left)),
        (rows_down, rows_north, (down, my_x)),
        (to_east.at[first_rows], west.at[high_halo], (down, right)),
        (to_west.at[first_rows], east.at[high_halo], (down, left)),
    ]
    copies = [
        pltpu.make_async_remote_copy(
            src_ref=source,
            dst_ref=target,
            send_sem=send_sem.at[which],
            recv_sem=recv_sem.at[which],
            device_id=device,
            device_id_type=MESH,
        )
        for which, (source, target, device) in enumerate(plan)
    ]
    beside, upward, downward = copies[0:2], copies[2:5], copies[5:8]

    def each(items, act):
        for item in items:
            act(item)

    start, wait_recv, wait_send = (lambda c: c.start()), (lambda c: c.wait_recv()), (lambda c: c.wait_send())
    pl.when(north_here)(lambda: each(upward[1:], start))
    pl.when(south_here)(lambda: each(downward[1:], start))
    each(beside, start)
    pl.when(north_here)(lambda: each(upward[:1], start))
    pl.when(south_here)(lambda: each(downward[:1], start))
    if rounds:
        tell(0)

    thick.wait()
    depth = col_in[...].astype(jnp.float32)
    faces[0] = jnp.minimum(depth, roll(depth, -1, 1))
    faces[1] = jnp.minimum(depth, roll(depth, -1, 0))
    own_sum[...] = jnp.zeros((rows, cols), jnp.float32)

    def level(k, carry):
        below = lax.convert_element_type(k, jnp.float32)
        current = transport(fields[0, k], fields[1, k], fields[2, k], faces[0] > below, faces[1] > below)
        tracer_out[k] = current
        own_sum[...] += jnp.where(col_in[...] > k, thickness[k] * current, 0.0)
        return carry

    lax.fori_loop(0, levels, level, 0, unroll=2)

    def blank(rows_ref, halo):
        rows_ref[...] = jnp.zeros(rows_ref.shape, jnp.float32)
        for ref in (west, east):
            ref[halo] = jnp.zeros((SUB, LANE), jnp.float32)

    pl.when(jnp.logical_not(south_here))(lambda: blank(rows_south, low_halo))
    pl.when(jnp.logical_not(north_here))(lambda: blank(rows_north, high_halo))

    for turn in range(1, len(rounds)):
        hear(turn - 1)
        tell(turn)
    pl.when(south_here)(lambda: each(upward[:1], wait_recv))
    pl.when(north_here)(lambda: each(downward[:1], wait_recv))

    def at(start):
        return slice(start, start + SUB)

    lane = iota((SUB, LANE), 1)
    group = lane // SEAM
    seat = lane % SEAM
    low_half = lane < LANE // 2

    def beyond(values, step):
        turned = [roll(v, -step, 1) for v in values]
        near = lane < LANE - 1 if step > 0 else lane > 0
        return [jnp.where(near, t, turned[(b + step) % len(values)]) for b, t in enumerate(turned)]

    def receive_south(k):
        for b in blocks:
            first, second = rows_south[k, b, 0:SUB], rows_south[k, b, SUB : 2 * SUB]
            yield first, second, jnp.where(sub < 6, roll(first, 3, 0), roll(second, -2, 0))

    def receive_north(k):
        for b in blocks:
            first, second = rows_north[k, b, 0:SUB], rows_north[k, b, SUB : 2 * SUB]
            yield first, second, jnp.where(sub < 3, roll(first, -5, 0), roll(second, -1, 0))

    for b in blocks:
        spare = [rows_south[k, b, SUB : 2 * SUB] for k in range(7)]
        flat[0, b, low_halo] = jnp.where(
            sub < 5, roll(spare[0], 1, 0), jnp.where(sub < 7, roll(spare[1], 3, 0), roll(spare[2], 5, 0))
        )
        for f in (1, 2):
            flat[f, b, low_halo] = jnp.where(sub < 7, roll(spare[2 * f + 1], 3, 0), roll(spare[2 * f + 2], 5, 0))
        spare = [rows_north[k, b, SUB : 2 * SUB] for k in range(4)]
        flat[0, b, high_halo] = jnp.where(sub < 3, roll(spare[0], -5, 0), roll(spare[1], -2, 0))
        for f in (1, 2):
            flat[f, b, high_halo] = roll(spare[f + 1], -5, 0)
        scale[b] = 1.0 / (6.0 + flat[1, b, 0 : rows + 2 * SUB])
    depth_lanes = (LANE - SUB + seat) % LANE
    for halo in (low_halo, high_halo):
        own_tile[3, halo] = pick(jnp.where(low_half, flat[0, 0, halo], flat[0, side_block - 1, halo]), depth_lanes)

    row_sides = ((0, receive_south, 0, SUB, 0, low_halo), (1, receive_north, SUB, 0, rows, high_halo))
    for w, receive, halo_at, own_at, base, halo in row_sides:
        open_east, open_nort = [], []
        for r in (0, SUB):
            deep = [flat[0, b, at(base + r)] for b in blocks]
            open_east.append([jnp.minimum(d, e) for d, e in zip(deep, beyond(deep, 1))])
            ahead = [flat[0, b, at(base + r + 1)] for b in blocks]
            open_nort.append([jnp.minimum(d, a) for d, a in zip(deep, ahead)])
        packed = [None] * 3
        own_rows = pl.ds(0, SUB) if w == 0 else pl.ds(rows - SUB, SUB)
        for k in range(levels):
            got = list(receive(k))
            for f in range(3):
                moved = roll(jnp.where(low_half, got[0][f], got[-1][f]), SEAM * k + SUB, 1)
                packed[f] = moved if packed[f] is None else jnp.where(group == k, moved, packed[f])
            for b in blocks:
                for r, values in (
                    (halo_at, got[b]),
                    (own_at, [fields[f, k, own_rows, LANE * b : LANE * (b + 1)] for f in range(3)]),
                ):
                    t = r // SUB
                    row_strips[w, 0, k, b, at(r)] = values[0]
                    row_strips[w, 1, k, b, at(r)] = jnp.where(open_east[t][b] > k, values[1], 0.0)
                    row_strips[w, 2, k, b, at(r)] = jnp.where(open_nort[t][b] > k, values[2], 0.0)
        for f in range(3):
            own_tile[f, halo] = packed[f]

    def row_step(w, f, k, r):
        here, ahead, behind = ([row_strips[w, f, k, b, at(r + d)] for b in blocks] for d in (0, 1, -1))
        fast_east, fast_north = ([row_strips[w, g, k, b, at(r)] for b in blocks] for g in (1, 2))
        fast_south = [row_strips[w, 2, k, b, at(r - 1)] for b in blocks]
        flux_east = [v * jnp.where(v > 0.0, c, x) for v, c, x in zip(fast_east, here, beyond(here, 1))]
        out = []
        for b, flux_west in enumerate(beyond(flux_east, -1)):
            flux_north = fast_north[b] * jnp.where(fast_north[b] > 0.0, here[b], ahead[b])
            flux_south = fast_south[b] * jnp.where(fast_south[b] > 0.0, behind[b], here[b])
            out.append(here[b] - (flux_east[b] - flux_west + flux_north - flux_south))
        return out

    for k in range(levels):
        for w in range(2):
            for b, new in enumerate(row_step(w, 0, k, SUB - 4)):
                row_strips[w, 3, k, b, at(SUB - 4)] = new
    row_sums = [[jnp.zeros((SUB, LANE), jnp.float32) for _ in blocks] for _ in range(2)]
    for k in range(levels):
        for w, base in enumerate((0, rows)):
            for b, new in enumerate(row_step(w, 3, k, SUB - 3)):
                row_strips[w, 4, k, b, at(SUB - 3)] = new
                row_sums[w][b] += jnp.where(flat[0, b, at(base + SUB - 3)] > k, thickness[k] * new, 0.0)
    for b in blocks:
        level_sum[b, inside] = own_sum[:, LANE * b : LANE * (b + 1)]
        level_sum[b, SUB - 3 : SUB + 2] = row_sums[0][b][0:5]
        level_sum[b, rows + SUB - 2 : rows + SUB + 3] = row_sums[1][b][1:6]

    strip_level = group.astype(jnp.float32)
    lane_thickness = jnp.zeros((SUB, LANE), jnp.float32)
    for k in range(levels):
        lane_thickness = jnp.where(group == k, thickness[k], lane_thickness)
    def side_lanes(base_west, base_east):
        return spare_lane(jnp.where(low_half, base_east + (lane & 3), base_west + ((lane - (LANE - 3)) & 3)))

    side_pick = [side_lanes(*bases) for bases in ((2, 0), (6, 6), (10, 10))]
    sides = []
    for got, shifts, first, in_halo in (
        (west, (3, -2, -6), 3, seat < SUB),
        (east, (8, 3, -2), 8, seat >= SUB),
    ):
        depth_pick = spare_lane(jnp.minimum(jnp.maximum(seat - first, 0), 4))
        sides.append((got, shifts, depth_pick, in_halo))

    each(beside, wait_recv)
    pl.when(south_here)(lambda: each(upward[1:], wait_recv))
    pl.when(north_here)(lambda: each(downward[1:], wait_recv))

    for r in range(0, rows + 2 * SUB, SUB):
        for w, (got, shifts, depth_pick, in_halo) in enumerate(sides):
            sent = got[at(r)]
            moved = [roll(sent, shift, 1) for shift in shifts] + [pick(sent, depth_pick)]
            for f in range(4):
                strips[w, f, at(r)] = jnp.where(in_halo, moved[f], own_tile[f, at(r)])
    for r in range(0, rows + 2 * SUB, SUB):
        for w in range(2):
            deep = strips[w, 3, at(r)]
            open_east = jnp.minimum(deep, roll(deep, -1, 1)) > strip_level
            open_nort = jnp.minimum(deep, strips[w, 3, at(r + 1)]) > strip_level
            strips[w, 1, at(r)] = jnp.where(open_east, strips[w, 1, at(r)], 0.0)
            strips[w, 2, at(r)] = jnp.where(open_nort, strips[w, 2, at(r)], 0.0)

    def side_step(w, f, r):
        here, ahead, behind = (strips[w, f, at(r + d)] for d in (0, 1, -1))
        fast_east, fast_north, fast_south = strips[w, 1, at(r)], strips[w, 2, at(r)], strips[w, 2, at(r - 1)]
        flux_east = fast_east * jnp.where(fast_east > 0.0, here, roll(here, -1, 1))
        flux_north = fast_north * jnp.where(fast_north > 0.0, here, ahead)
        flux_south = fast_south * jnp.where(fast_south > 0.0, behind, here)
        return here - (flux_east - roll(flux_east, 1, 1) + flux_north - flux_south)

    for r in range(SUB - 4, rows + SUB + 4, SUB):
        for w in range(2):
            strips[w, 4, at(r)] = side_step(w, 0, r)
    inner_rows = range(SUB - 3, rows + SUB + 3, SUB)
    for r in inner_rows:
        for w in range(2):
            new = side_step(w, 4, r)
            strips[w, 5, at(r)] = new
            strips[w, 0, at(r)] = jnp.where(strips[w, 3, at(r)] > strip_level, lane_thickness * new, 0.0)
    for f, lanes in enumerate(side_pick):
        for r in range(0, rows + 2 * SUB, SUB):
            flat[f, side_block, at(r)] = jnp.where(low_half, pick(east[at(r)], lanes), pick(west[at(r)], lanes))
    for r in inner_rows:
        for w in range(2):
            total = strips[w, 0, at(r)]
            strips[w, 1, at(r)] = total + roll(total, LANE // 2, 1)
    for r in inner_rows:
        for w in range(2):
            total = strips[w, 1, at(r)]
            strips[w, 2, at(r)] = sum(roll(total, shift - SUB, 1) for shift in range(0, LANE // 2, SEAM))
    for r in inner_rows:
        sum_west, sum_east = strips[0, 2, at(r)], strips[1, 2, at(r)]
        for b in range(side_block + 1):
            if b < side_block:
                total, inverse = level_sum[b, at(r)], scale[b, at(r)]
                if b == 0:
                    total = jnp.where(lane < 2, sum_west, total)
                if b == side_block - 1:
                    total = jnp.where(lane >= LANE - 2, sum_east, total)
            else:
                total = jnp.where(low_half, sum_east, sum_west)
                inverse = 1.0 / (6.0 + flat[1, b, at(r)])
            z0 = (flat[2, b, at(r)] + total) * inverse
            if b < side_block:
                level_sum[b, at(r)] = z0
            wet = flat[0, b, at(r)] > 0.0
            scale[b, at(r)] = jnp.where(wet, inverse, 0.0)
            start_vec[0, b, at(r)] = jnp.where(wet, z0, 0.0)

    def off_diagonal(source, r, wanted):
        upright, mixed = [], []
        for b in range(side_block + 1):
            both = start_vec[source, b, at(r - 1)] + start_vec[source, b, at(r + 1)]
            upright.append(both)
            mixed.append(start_vec[source, b, at(r)] + 0.5 * both)
        ahead, behind = ([roll(m, d, 1) for m in mixed] for d in (-1, 1))
        out = []
        for b in range(wanted):
            after = jnp.where(lane < LANE - 1, ahead[b], ahead[(b + 1) % (side_block + 1)])
            before = jnp.where(lane > 0, behind[b], behind[b - 1])
            out.append(scale[b, at(r)] * (upright[b] + after + before))
        return out

    for power in (1, 2):
        for r in range(SUB - 3 + power, rows + SUB + 3 - power, SUB):
            for b, z in enumerate(off_diagonal(power - 1, r, side_block + 1)):
                start_vec[power, b, at(r)] = z

    sums = [jnp.zeros((SUB, LANE), jnp.float32)] * (2 * ITERS)
    for r in range(SUB, rows + SUB, SUB):
        for b, z3 in enumerate(off_diagonal(2, r, side_block)):
            z = [level_sum[b, at(r)], start_vec[1, b, at(r)], start_vec[2, b, at(r)], z3]
            for i in range(ITERS):
                basis_out[i, b, at(r - SUB)] = z[i]
                scaled = (6.0 + flat[1, b, at(r)]) * z[i]
                sums[2 * i] += scaled * z[i]
                sums[2 * i + 1] += scaled * z[i + 1]
    sums = [jnp.sum(total, axis=0, keepdims=True) for total in sums]
    folded = jnp.concatenate(sums + [jnp.zeros((SUB - len(sums), LANE), jnp.float32)], axis=0)
    diag = iota((SUB, LANE), 1) == iota((SUB, LANE), 0)
    folded = jnp.sum(folded, axis=1, keepdims=True)
    part[...] = jnp.sum(jnp.where(diag, folded, 0.0), axis=0, keepdims=True)

    if rounds:
        hear(len(rounds) - 1)
    for index, target in enumerate(others):
        pltpu.make_async_remote_copy(
            src_ref=part,
            dst_ref=slots.at[index],
            send_sem=sum_send_sem,
            recv_sem=sum_recv_sem,
            device_id=target,
            device_id_type=MESH,
        ).start()

    for k in range(levels):
        for b in blocks:
            here = slice(LANE * b, LANE * (b + 1))
            tracer_out[k, 0:2, here] = row_strips[0, 4, k, b, SUB : SUB + 2]
            tracer_out[k, rows - 2 : rows, here] = row_strips[1, 4, k, b, SUB - 2 : SUB]
    lane = iota((rows, LANE), 1)
    side_new = jnp.where(lane % SEAM < SUB, strips[1, 5, inside], strips[0, 5, inside])
    for k in range(levels):
        moved = roll(side_new, -SEAM * k - SUB, 1)
        tracer_out[k, :, 0:LANE] = jnp.where(lane < 2, moved, tracer_out[k, :, 0:LANE])
        tracer_out[k, :, cols - LANE : cols] = jnp.where(lane >= LANE - 2, moved, tracer_out[k, :, cols - LANE : cols])

    everything = pltpu.make_async_remote_copy(
        src_ref=slots,
        dst_ref=slots,
        send_sem=sum_send_sem,
        recv_sem=sum_recv_sem,
        device_id=others[0],
        device_id_type=MESH,
    )
    everything.wait_recv()
    moments_out[...] = jnp.sum(slots[...], axis=0) + part[...]

    everything.wait_send()
    each(beside, wait_send)
    pl.when(north_here)(lambda: each(upward, wait_send))
    pl.when(south_here)(lambda: each(downward, wait_send))


def finish(tracer_ref, basis_ref, moments_ref, tracer_out, heights_out, heights, save):
    levels = tracer_ref.shape[0]
    saves = [pltpu.make_async_copy(tracer_ref.at[k], tracer_out.at[k], save.at[k]) for k in range(levels)]
    for copy in saves:
        copy.start()
    diag = iota((SUB, LANE), 1) == iota((SUB, LANE), 0)
    total = jnp.broadcast_to(moments_ref[...], (SUB, LANE))
    total = jnp.sum(jnp.where(diag, total, 0.0), axis=1, keepdims=True)
    moment = [total[i : i + 1, :] for i in range(2 * ITERS)]

    def inner(a, b):
        return sum(x * y * moment[i + j] for i, x in enumerate(a) for j, y in enumerate(b))

    def ratio(top, bottom):
        good = bottom > 0.0
        return jnp.where(good, top / jnp.where(good, bottom, 1.0), 0.0)

    one, zero = jnp.ones((1, 1), jnp.float32), jnp.zeros((1, 1), jnp.float32)
    scaled, direction, height = [one], [one], [zero] * ITERS
    product_now = moment[0]
    for iteration in range(ITERS):
        low, high = direction + [zero], [zero] + direction
        applied = [a - b for a, b in zip(low, high)]
        step_size = ratio(product_now, inner(direction, applied))
        for i, x in enumerate(direction):
            height[i] = height[i] + step_size * x
        if iteration + 1 < ITERS:
            scaled = [a - step_size * b for a, b in zip(scaled + [zero], applied)]
            product_next = jnp.maximum(inner(scaled, scaled), 0.0)
            factor = ratio(product_next, product_now)
            direction = [a + factor * b for a, b in zip(scaled, low)]
            product_now = product_next
    for b in range(basis_ref.shape[1]):
        heights[:, LANE * b : LANE * (b + 1)] = sum(h * basis_ref[i, b] for i, h in enumerate(height))

    saves.append(pltpu.make_async_copy(heights, heights_out, save.at[levels]))
    saves[-1].start()
    for copy in saves:
        copy.wait()


def on_device(ny, nx, tracer, east_speed, north_speed, columns, thickness, surface_flux, helm):
    levels, rows, cols = tracer.shape
    hbm = pl.BlockSpec(memory_space=pl.ANY)
    vmem = pl.BlockSpec(memory_space=pltpu.VMEM)
    f32 = jnp.float32
    dma = pltpu.SemaphoreType.DMA
    blocks = cols // LANE
    tall = rows + 2 * SUB
    scratch = [
        pltpu.VMEM((3, levels, rows, cols), f32),
        pltpu.VMEM((rows, cols), jnp.int32),
        pltpu.VMEM((3, blocks + 1, tall + SUB, LANE), f32),
        pltpu.VMEM((4, tall, LANE), f32),
        *[pltpu.VMEM((rows, LANE), f32)] * 2,
        *[pltpu.VMEM((tall, LANE), f32)] * 2,
        *[pltpu.VMEM((levels, blocks, 2 * SUB, LANE), f32)] * 4,
        pltpu.VMEM((2, 5, levels, blocks, 2 * SUB, LANE), f32),
        pltpu.VMEM((rows, cols), f32),
        pltpu.VMEM((2, rows, cols), f32),
        pltpu.VMEM((2, 6, tall + SUB, LANE), f32),
        pltpu.VMEM((blocks + 1, tall, LANE), f32),
        pltpu.VMEM((blocks + 1, tall, LANE), f32),
        pltpu.VMEM((ITERS, blocks + 1, tall + SUB, LANE), f32),
        pltpu.VMEM((1, LANE), f32),
        pltpu.VMEM((ny * nx - 1, 1, LANE), f32),
        pltpu.SMEM((levels,), f32),
        pltpu.SemaphoreType.REGULAR((max(ny, nx).bit_length(),)),
        dma((7 + 2 * blocks,)),
        dma((8,)),
        dma((8,)),
        dma,
        dma,
    ]
    results = pl.pallas_call(
        functools.partial(kernel, ny, nx),
        out_shape=(
            pltpu.VMEM((levels, rows, cols), f32),
            pltpu.VMEM((ITERS, blocks, rows, LANE), f32),
            pltpu.VMEM((1, LANE), f32),
        ),
        in_specs=[hbm] * 7,
        out_specs=(vmem,) * 3,
        scratch_shapes=scratch,
        compiler_params=pltpu.CompilerParams(collective_id=0, has_side_effects=True),
    )(tracer, east_speed, north_speed, columns, thickness, surface_flux, helm)
    return pl.pallas_call(
        finish,
        out_shape=(
            jax.ShapeDtypeStruct((levels, rows, cols), f32),
            jax.ShapeDtypeStruct((rows, cols), f32),
        ),
        in_specs=[vmem] * 3,
        out_specs=(hbm, hbm),
        scratch_shapes=[pltpu.VMEM((rows, cols), f32), dma((levels + 1,))],
    )(*[pltpu.with_memory_space_constraint(r, pltpu.VMEM) for r in results])


def solution(mesh):
    spec = P(None, "gy", "gx")
    flat = P("gy", "gx")
    return jax.shard_map(
        functools.partial(on_device, mesh.shape["gy"], mesh.shape["gx"]),
        mesh=mesh,
        in_specs=(spec, spec, spec, flat, P(), flat, flat),
        out_specs=(spec, flat),
        check_vma=False,
    )
```

```python
import functools

import jax
import jax.numpy as jnp
from jax import lax
from jax.experimental import pallas as pl
from jax.experimental.pallas import tpu as pltpu
from jax.sharding import PartitionSpec as P

TSTEPS = 2
ITERS = 3
MESH = pl.DeviceIdType.MESH
SUB = 8
LANE = 128
SEAM = 16


def roll(array, shift, axis):
    shift = shift % array.shape[axis]
    return pltpu.roll(array, shift, axis) if shift else array


def iota(shape, dim):
    return lax.broadcasted_iota(jnp.int32, shape, dim)


def pick(array, lanes):
    return jnp.take_along_axis(array, lanes, axis=1, mode="promise_in_bounds")


def transport(current, east, nort, open_east, open_nort):
    east = jnp.where(open_east, east, 0.0)
    nort = jnp.where(open_nort, nort, 0.0)
    for _ in range(TSTEPS):
        flux_east = east * jnp.where(east > 0.0, current, roll(current, -1, 1))
        flux_north = nort * jnp.where(nort > 0.0, current, roll(current, -1, 0))
        current = current - (flux_east - roll(flux_east, 1, 1) + flux_north - roll(flux_north, 1, 0))
    return current


def kernel(
    ny,
    nx,
    tracer_ref,
    east_ref,
    north_ref,
    columns_ref,
    thick_hbm,
    surface_ref,
    helm_ref,
    tracer_out,
    basis_out,
    moments_out,
    fields,
    col_in,
    flat,
    own_tile,
    to_east,
    to_west,
    west,
    east,
    rows_up,
    rows_down,
    rows_south,
    rows_north,
    row_strips,
    own_sum,
    faces,
    strips,
    level_sum,
    scale,
    start_vec,
    part,
    slots,
    thickness,
    know_sem,
    in_sem,
    send_sem,
    recv_sem,
    sum_send_sem,
    sum_recv_sem,
):
    _, levels, rows, cols = fields.shape
    my_y, my_x = lax.axis_index("gy"), lax.axis_index("gx")

    def wrap(value, size):
        return jnp.where(value >= size, value - size, value)

    ys = [my_y] + [wrap(my_y + d, ny) for d in range(1, ny)]
    xs = [my_x] + [wrap(my_x + d, nx) for d in range(1, nx)]
    others = [(y, x) for b, x in enumerate(xs) for a, y in enumerate(ys) if a or b]
    south_here, north_here = my_y > 0, my_y < ny - 1

    blocks = range(cols // LANE)
    side_block = cols // LANE
    inside = pl.ds(SUB, rows)
    small = [pltpu.make_async_copy(columns_ref, col_in, in_sem.at[0])] + [
        pltpu.make_async_copy(ref.at[:, pl.ds(LANE * b, LANE)], flat.at[f, b, inside], in_sem.at[1 + len(blocks) * (f - 1) + b])
        for f, ref in ((1, helm_ref), (2, surface_ref))
        for b in blocks
    ]
    halves = [range(0, levels // 2), range(levels // 2, levels)]
    large = [
        [
            pltpu.make_async_copy(
                ref.at[pl.ds(half[0], len(half))],
                fields.at[f, pl.ds(half[0], len(half))],
                in_sem.at[1 + 2 * len(blocks) + 2 * f + h],
            )
            for h, half in enumerate(halves)
        ]
        for f, ref in enumerate((tracer_ref, east_ref, north_ref))
    ]
    thick = pltpu.make_async_copy(thick_hbm, thickness, in_sem.at[7 + 2 * len(blocks)])
    for load in small + sum(large, []) + [thick]:
        load.start()
    barrier = pltpu.get_barrier_semaphore()

    def around(reach_y, reach_x):
        return [(ys[a], xs[b]) for a in reach_y for b in reach_x if a or b]

    def reach(distance, known, size):
        return (0,) if 2 * known + 1 >= size else (distance, -distance, 0)

    greeted = around(reach(1, 0, ny), reach(1, 0, nx))
    for target in greeted:
        pl.semaphore_signal(barrier, inc=1, device_id=target, device_id_type=MESH)
    rounds, known = [], 1
    while 2 * known + 1 < max(ny, nx):
        rounds.append(around(reach(known, known, ny), reach(known, known, nx)))
        known *= 2

    def tell(turn):
        for target in rounds[turn]:
            pl.semaphore_signal(know_sem.at[turn], inc=1, device_id=target, device_id_type=MESH)

    def hear(turn):
        pl.semaphore_wait(know_sem.at[turn], len(rounds[turn]))


    lane = iota((rows, LANE), 1)
    group = lane // SEAM
    seat = lane % SEAM
    first_rows, last_rows = pl.ds(0, SUB), pl.ds(rows - SUB, SUB)
    low_halo, low_own, high_own, high_halo = (pl.ds(at, SUB) for at in (0, SUB, rows, rows + SUB))

    def both_edges(left, right):
        return jnp.where(lane < LANE // 2, left, right)

    def flat_edges(f):
        return both_edges(flat[f, 0, inside], flat[f, side_block - 1, inside])

    def spare_lane(slot):
        return SEAM * (slot // 2) + SEAM - 2 + slot % 2

    for load in small:
        load.wait()
    for b in blocks:
        flat[0, b, inside] = col_in[:, LANE * b : LANE * (b + 1)].astype(jnp.float32)
    depth_edge = flat_edges(0)
    own_tile[3, inside] = pick(depth_edge, (LANE - SUB + seat) % LANE)
    three = jnp.where(
        (lane < SUB) | (lane >= LANE - SUB),
        depth_edge,
        jnp.where(lane < 3 * SUB, roll(flat_edges(1), 2 * SUB, 1), roll(flat_edges(2), 4 * SUB, 1)),
    )
    slot = jnp.maximum(2 * group + seat - (SEAM - 2), 0)
    east_from = jnp.where(slot < 6, LANE - 5 + slot, jnp.where(slot < 10, slot - 6 + 13, slot - 10 + 29)) % LANE
    west_from = jnp.where(slot < 6, slot, jnp.where(slot < 10, slot - 6 + 16, slot - 10 + 32)) % LANE
    spare_east, spare_west = pick(three, east_from), pick(three, west_from)
    sub = iota((SUB, LANE), 0)
    spare_up = ((0, -1), (0, -3), (0, -5), (1, -3), (1, -5), (2, -3), (2, -5))
    spare_down = ((0, 5), (0, 2), (1, 5), (2, 5))

    def spare_rows(which, k, b, where):
        field, turn = which[min(k, len(which) - 1)]
        return roll(flat[field, b, where], turn, 0)

    def pack_rows(k):
        for b in blocks:
            here = slice(LANE * b, LANE * (b + 1))
            c, e, n = (fields[f, k, rows - SUB : rows, here] for f in range(3))
            rows_up[k, b, 0:SUB] = jnp.where(sub < 3, roll(n, -3, 0), c)
            rows_up[k, b, SUB : 2 * SUB] = jnp.where(
                sub < 2, roll(n, 2, 0), jnp.where(sub < 4, spare_rows(spare_up, k, b, high_own), e)
            )
            c, e, n = (fields[f, k, 0:SUB, here] for f in range(3))
            rows_down[k, b, 0:SUB] = jnp.where(sub < 5, c, roll(n, 5, 0))
            rows_down[k, b, SUB : 2 * SUB] = jnp.where(
                sub < 4, e, jnp.where(sub < 5, roll(n, 1, 0), spare_rows(spare_down, k, b, low_own))
            )

    starts = (0, 5, 10, SEAM - 2)
    for f, (shift_east, shift_west) in enumerate(((-3, -8), (2, -3), (6, 2))):
        packed = None
        for h, half in enumerate(halves):
            large[f][h].wait()
            for k in half:
                both = both_edges(fields[f, k, :, 0:LANE], fields[f, k, :, cols - LANE : cols])
                moved = roll(both, SEAM * k + SUB, 1)
                packed = moved if packed is None else jnp.where(group == k, moved, packed)
            if f == 2:
                for k in half:
                    pack_rows(k)
        own_tile[f, inside] = packed
        seats = (seat >= starts[f]) & (seat < starts[f + 1])
        to_east[...] = jnp.where(seats, roll(packed, shift_east, 1), spare_east if f == 0 else to_east[...])
        to_west[...] = jnp.where(seats, roll(packed, shift_west, 1), spare_west if f == 0 else to_west[...])

    pl.semaphore_wait(barrier, len(greeted))

    up, down, right, left = wrap(my_y + 1, ny), wrap(my_y + ny - 1, ny), xs[1], xs[-1]
    plan = [
        (to_east, west.at[inside], (my_y, right)),
        (to_west, east.at[inside], (my_y, left)),
        (rows_up, rows_south, (up, my_x)),
        (to_east.at[last_rows], west.at[low_halo], (up, right)),
        (to_west.at[last_rows], east.at[low_halo], (up, left)),
        (rows_down, rows_north, (down, my_x)),
        (to_east.at[first_rows], west.at[high_halo], (down, right)),
        (to_west.at[first_rows], east.at[high_halo], (down, left)),
    ]
    copies = [
        pltpu.make_async_remote_copy(
            src_ref=source,
            dst_ref=target,
            send_sem=send_sem.at[which],
            recv_sem=recv_sem.at[which],
            device_id=device,
            device_id_type=MESH,
        )
        for which, (source, target, device) in enumerate(plan)
    ]
    beside, upward, downward = copies[0:2], copies[2:5], copies[5:8]

    def each(items, act):
        for item in items:
            act(item)

    start, wait_recv, wait_send = (lambda c: c.start()), (lambda c: c.wait_recv()), (lambda c: c.wait_send())
    far_east, far_west = my_x == nx - 1, my_x == 0
    pl.when(north_here)(lambda: each(upward[1:], start))
    pl.when(south_here)(lambda: each(downward[1:], start))
    pl.when(far_east)(copies[0].start)
    pl.when(far_west)(copies[1].start)
    far_up, far_down = my_y == ny // 2 - 1, my_y == ny // 2
    pl.when(far_up)(upward[0].start)
    pl.when(far_down)(downward[0].start)
    if rounds:
        tell(0)

    thick.wait()
    depth = col_in[...].astype(jnp.float32)
    faces[0] = jnp.minimum(depth, roll(depth, -1, 1))
    faces[1] = jnp.minimum(depth, roll(depth, -1, 0))
    own_sum[...] = jnp.zeros((rows, cols), jnp.float32)

    def level(k, carry):
        below = lax.convert_element_type(k, jnp.float32)
        current = transport(fields[0, k], fields[1, k], fields[2, k], faces[0] > below, faces[1] > below)
        tracer_out[k] = current
        own_sum[...] += jnp.where(col_in[...] > k, thickness[k] * current, 0.0)
        return carry

    part_way = levels * 1 // 8
    lax.fori_loop(0, part_way, level, 0, unroll=2)
    pl.when(north_here & jnp.logical_not(far_up))(upward[0].start)
    pl.when(south_here & jnp.logical_not(far_down))(downward[0].start)
    pl.when(jnp.logical_not(far_east))(copies[0].start)
    pl.when(jnp.logical_not(far_west))(copies[1].start)
    lax.fori_loop(part_way, levels, level, 0, unroll=2)

    def blank(rows_ref, halo):
        rows_ref[...] = jnp.zeros(rows_ref.shape, jnp.float32)
        for ref in (west, east):
            ref[halo] = jnp.zeros((SUB, LANE), jnp.float32)

    pl.when(jnp.logical_not(south_here))(lambda: blank(rows_south, low_halo))
    pl.when(jnp.logical_not(north_here))(lambda: blank(rows_north, high_halo))

    for turn in range(1, len(rounds)):
        hear(turn - 1)
        tell(turn)
    pl.when(south_here)(lambda: each(upward[:1], wait_recv))
    pl.when(north_here)(lambda: each(downward[:1], wait_recv))

    def at(start):
        return slice(start, start + SUB)

    lane = iota((SUB, LANE), 1)
    group = lane // SEAM
    seat = lane % SEAM
    low_half = lane < LANE // 2

    def beyond(values, step):
        turned = [roll(v, -step, 1) for v in values]
        near = lane < LANE - 1 if step > 0 else lane > 0
        return [jnp.where(near, t, turned[(b + step) % len(values)]) for b, t in enumerate(turned)]

    def receive_south(k):
        for b in blocks:
            first, second = rows_south[k, b, 0:SUB], rows_south[k, b, SUB : 2 * SUB]
            yield first, second, jnp.where(sub < 6, roll(first, 3, 0), roll(second, -2, 0))

    def receive_north(k):
        for b in blocks:
            first, second = rows_north[k, b, 0:SUB], rows_north[k, b, SUB : 2 * SUB]
            yield first, second, jnp.where(sub < 3, roll(first, -5, 0), roll(second, -1, 0))

    for b in blocks:
        spare = [rows_south[k, b, SUB : 2 * SUB] for k in range(7)]
        flat[0, b, low_halo] = jnp.where(
            sub < 5, roll(spare[0], 1, 0), jnp.where(sub < 7, roll(spare[1], 3, 0), roll(spare[2], 5, 0))
        )
        for f in (1, 2):
            flat[f, b, low_halo] = jnp.where(sub < 7, roll(spare[2 * f + 1], 3, 0), roll(spare[2 * f + 2], 5, 0))
        spare = [rows_north[k, b, SUB : 2 * SUB] for k in range(4)]
        flat[0, b, high_halo] = jnp.where(sub < 3, roll(spare[0], -5, 0), roll(spare[1], -2, 0))
        for f in (1, 2):
            flat[f, b, high_halo] = roll(spare[f + 1], -5, 0)
        scale[b] = 1.0 / (6.0 + flat[1, b, 0 : rows + 2 * SUB])
    depth_lanes = (LANE - SUB + seat) % LANE
    for halo in (low_halo, high_halo):
        own_tile[3, halo] = pick(jnp.where(low_half, flat[0, 0, halo], flat[0, side_block - 1, halo]), depth_lanes)
    for r in range(0, rows + 2 * SUB, SUB):
        own_tile[4, at(r)] = roll(own_tile[3, at(r)], -1, 1)

    row_sides = ((0, receive_south, 0, SUB, 0, low_halo), (1, receive_north, SUB, 0, rows, high_halo))
    for w, receive, halo_at, own_at, base, halo in row_sides:
        open_east, open_nort = [], []
        for r in (0, SUB):
            deep = [flat[0, b, at(base + r)] for b in blocks]
            open_east.append([jnp.minimum(d, e) for d, e in zip(deep, beyond(deep, 1))])
            ahead = [flat[0, b, at(base + r + 1)] for b in blocks]
            open_nort.append([jnp.minimum(d, a) for d, a in zip(deep, ahead)])
        packed = [None] * 3
        own_rows = pl.ds(0, SUB) if w == 0 else pl.ds(rows - SUB, SUB)
        for k in range(levels):
            got = list(receive(k))
            for f in range(3):
                moved = roll(jnp.where(low_half, got[0][f], got[-1][f]), SEAM * k + SUB, 1)
                packed[f] = moved if packed[f] is None else jnp.where(group == k, moved, packed[f])
            for b in blocks:
                for r, values in (
                    (halo_at, got[b]),
                    (own_at, [fields[f, k, own_rows, LANE * b : LANE * (b + 1)] for f in range(3)]),
                ):
                    t = r // SUB
                    row_strips[w, 0, k, b, at(r)] = values[0]
                    row_strips[w, 1, k, b, at(r)] = jnp.where(open_east[t][b] > k, values[1], 0.0)
                    row_strips[w, 2, k, b, at(r)] = jnp.where(open_nort[t][b] > k, values[2], 0.0)
        for f in range(3):
            own_tile[f, halo] = packed[f]

    def row_step(w, f, k, r):
        here, ahead, behind = ([row_strips[w, f, k, b, at(r + d)] for b in blocks] for d in (0, 1, -1))
        fast_east, fast_north = ([row_strips[w, g, k, b, at(r)] for b in blocks] for g in (1, 2))
        fast_south = [row_strips[w, 2, k, b, at(r - 1)] for b in blocks]
        flux_east = [v * jnp.where(v > 0.0, c, x) for v, c, x in zip(fast_east, here, beyond(here, 1))]
        out = []
        for b, flux_west in enumerate(beyond(flux_east, -1)):
            flux_north = fast_north[b] * jnp.where(fast_north[b] > 0.0, here[b], ahead[b])
            flux_south = fast_south[b] * jnp.where(fast_south[b] > 0.0, behind[b], here[b])
            out.append(here[b] - (flux_east[b] - flux_west + flux_north - flux_south))
        return out

    for k in range(levels):
        for w in range(2):
            for b, new in enumerate(row_step(w, 0, k, SUB - 4)):
                row_strips[w, 3, k, b, at(SUB - 4)] = new
    row_sums = [[jnp.zeros((SUB, LANE), jnp.float32) for _ in blocks] for _ in range(2)]
    for k in range(levels):
        for w, base in enumerate((0, rows)):
            for b, new in enumerate(row_step(w, 3, k, SUB - 3)):
                row_strips[w, 4, k, b, at(SUB - 3)] = new
                row_sums[w][b] += jnp.where(flat[0, b, at(base + SUB - 3)] > k, thickness[k] * new, 0.0)
    for b in blocks:
        level_sum[b, inside] = own_sum[:, LANE * b : LANE * (b + 1)]
        level_sum[b, SUB - 3 : SUB + 2] = row_sums[0][b][0:5]
        level_sum[b, rows + SUB - 2 : rows + SUB + 3] = row_sums[1][b][1:6]

    strip_level = group.astype(jnp.float32)
    lane_thickness = jnp.zeros((SUB, LANE), jnp.float32)
    for k in range(levels):
        lane_thickness = jnp.where(group == k, thickness[k], lane_thickness)
    def side_lanes(base_west, base_east):
        return spare_lane(jnp.where(low_half, base_east + (lane & 3), base_west + ((lane - (LANE - 3)) & 3)))

    side_pick = [side_lanes(*bases) for bases in ((2, 0), (6, 6), (10, 10))]
    sides = []
    for got, shifts, first, in_halo in (
        (west, (3, -2, -6), 3, [seat + d < SUB for d in (0, 1)]),
        (east, (8, 3, -2), 8, [seat + d >= SUB for d in (0, 1)]),
    ):
        depth_picks = [spare_lane(jnp.minimum(jnp.maximum(seat + d - first, 0), 4)) for d in (0, 1)]
        sides.append((got, shifts, depth_picks, in_halo))

    each(beside, wait_recv)
    pl.when(south_here)(lambda: each(upward[1:], wait_recv))
    pl.when(north_here)(lambda: each(downward[1:], wait_recv))

    tall_rows = range(0, rows + 2 * SUB, SUB)
    for w, (got, shifts, depth_picks, in_halo) in enumerate(sides):
        for d, lanes in enumerate(depth_picks):
            for r in tall_rows:
                strips[w, 3 + d, at(r)] = jnp.where(in_halo[d], pick(got[at(r)], lanes), own_tile[3 + d, at(r)])
    for f, lanes in enumerate(side_pick):
        for r in tall_rows:
            flat[f, side_block, at(r)] = jnp.where(low_half, pick(east[at(r)], lanes), pick(west[at(r)], lanes))
    for r in tall_rows:
        for w, (got, shifts, depth_picks, in_halo) in enumerate(sides):
            sent = got[at(r)]
            c, e, n = (jnp.where(in_halo[0], roll(sent, shift, 1), own_tile[f, at(r)]) for f, shift in enumerate(shifts))
            strips[w, 0, at(r)] = c
            strips[w, 1, at(r)] = jnp.where(jnp.minimum(strips[w, 3, at(r)], strips[w, 4, at(r)]) > strip_level, e, 0.0)
            strips[w, 2, at(r)] = n
    for r in range(0, rows + 2 * SUB, SUB):
        for w in range(2):
            open_nort = jnp.minimum(strips[w, 3, at(r)], strips[w, 3, at(r + 1)]) > strip_level
            strips[w, 2, at(r)] = jnp.where(open_nort, strips[w, 2, at(r)], 0.0)

    def side_step(w, f, r):
        here, ahead, behind = (strips[w, f, at(r + d)] for d in (0, 1, -1))
        fast_east, fast_north, fast_south = strips[w, 1, at(r)], strips[w, 2, at(r)], strips[w, 2, at(r - 1)]
        flux_east = fast_east * jnp.where(fast_east > 0.0, here, roll(here, -1, 1))
        flux_north = fast_north * jnp.where(fast_north > 0.0, here, ahead)
        flux_south = fast_south * jnp.where(fast_south > 0.0, behind, here)
        return here - (flux_east - roll(flux_east, 1, 1) + flux_north - flux_south)

    for r in range(SUB - 4, rows + SUB + 4, SUB):
        for w in range(2):
            strips[w, 4, at(r)] = side_step(w, 0, r)
    inner_rows = range(SUB - 3, rows + SUB + 3, SUB)
    for r in inner_rows:
        for w in range(2):
            new = side_step(w, 4, r)
            strips[w, 5, at(r)] = new
            strips[w, 0, at(r)] = jnp.where(strips[w, 3, at(r)] > strip_level, lane_thickness * new, 0.0)
    for r in inner_rows:
        for w in range(2):
            total = strips[w, 0, at(r)]
            strips[w, 1, at(r)] = total + roll(total, LANE // 2, 1)
    for r in inner_rows:
        for w in range(2):
            total = strips[w, 1, at(r)]
            strips[w, 2, at(r)] = sum(roll(total, shift - SUB, 1) for shift in range(0, LANE // 2, SEAM))
    for r in inner_rows:
        sum_west, sum_east = strips[0, 2, at(r)], strips[1, 2, at(r)]
        for b in range(side_block + 1):
            if b < side_block:
                total, inverse = level_sum[b, at(r)], scale[b, at(r)]
                if b == 0:
                    total = jnp.where(lane < 2, sum_west, total)
                if b == side_block - 1:
                    total = jnp.where(lane >= LANE - 2, sum_east, total)
            else:
                total = jnp.where(low_half, sum_east, sum_west)
                inverse = 1.0 / (6.0 + flat[1, b, at(r)])
            z0 = (flat[2, b, at(r)] + total) * inverse
            if b < side_block:
                level_sum[b, at(r)] = z0
            wet = flat[0, b, at(r)] > 0.0
            scale[b, at(r)] = jnp.where(wet, inverse, 0.0)
            start_vec[0, b, at(r)] = jnp.where(wet, z0, 0.0)

    def off_diagonal(source, r, wanted):
        upright, mixed = [], []
        for b in range(side_block + 1):
            both = start_vec[source, b, at(r - 1)] + start_vec[source, b, at(r + 1)]
            upright.append(both)
            mixed.append(start_vec[source, b, at(r)] + 0.5 * both)
        ahead, behind = ([roll(m, d, 1) for m in mixed] for d in (-1, 1))
        out = []
        for b in range(wanted):
            after = jnp.where(lane < LANE - 1, ahead[b], ahead[(b + 1) % (side_block + 1)])
            before = jnp.where(lane > 0, behind[b], behind[b - 1])
            out.append(scale[b, at(r)] * (upright[b] + after + before))
        return out

    for power in (1, 2):
        for r in range(SUB - 3 + power, rows + SUB + 3 - power, SUB):
            for b, z in enumerate(off_diagonal(power - 1, r, side_block + 1)):
                start_vec[power, b, at(r)] = z

    sums = [jnp.zeros((SUB, LANE), jnp.float32)] * (2 * ITERS)
    for r in range(SUB, rows + SUB, SUB):
        for b, z3 in enumerate(off_diagonal(2, r, side_block)):
            z = [level_sum[b, at(r)], start_vec[1, b, at(r)], start_vec[2, b, at(r)], z3]
            for i in range(ITERS):
                basis_out[i, b, at(r - SUB)] = z[i]
                scaled = (6.0 + flat[1, b, at(r)]) * z[i]
                sums[2 * i] += scaled * z[i]
                sums[2 * i + 1] += scaled * z[i + 1]
    sums = [jnp.sum(total, axis=0, keepdims=True) for total in sums]
    folded = jnp.concatenate(sums + [jnp.zeros((SUB - len(sums), LANE), jnp.float32)], axis=0)
    diag = iota((SUB, LANE), 1) == iota((SUB, LANE), 0)
    folded = jnp.sum(folded, axis=1, keepdims=True)
    part[...] = jnp.sum(jnp.where(diag, folded, 0.0), axis=0, keepdims=True)

    if rounds:
        hear(len(rounds) - 1)
    for index, target in enumerate(others):
        pltpu.make_async_remote_copy(
            src_ref=part,
            dst_ref=slots.at[index],
            send_sem=sum_send_sem,
            recv_sem=sum_recv_sem,
            device_id=target,
            device_id_type=MESH,
        ).start()

    for k in range(levels):
        for b in blocks:
            here = slice(LANE * b, LANE * (b + 1))
            tracer_out[k, 0:2, here] = row_strips[0, 4, k, b, SUB : SUB + 2]
            tracer_out[k, rows - 2 : rows, here] = row_strips[1, 4, k, b, SUB - 2 : SUB]
    lane = iota((rows, LANE), 1)
    side_new = jnp.where(lane % SEAM < SUB, strips[1, 5, inside], strips[0, 5, inside])
    for k in range(levels):
        moved = roll(side_new, -SEAM * k - SUB, 1)
        tracer_out[k, :, 0:LANE] = jnp.where(lane < 2, moved, tracer_out[k, :, 0:LANE])
        tracer_out[k, :, cols - LANE : cols] = jnp.where(lane >= LANE - 2, moved, tracer_out[k, :, cols - LANE : cols])

    everything = pltpu.make_async_remote_copy(
        src_ref=slots,
        dst_ref=slots,
        send_sem=sum_send_sem,
        recv_sem=sum_recv_sem,
        device_id=others[0],
        device_id_type=MESH,
    )
    everything.wait_recv()
    moments_out[...] = jnp.sum(slots[...], axis=0) + part[...]

    everything.wait_send()
    each(beside, wait_send)
    pl.when(north_here)(lambda: each(upward, wait_send))
    pl.when(south_here)(lambda: each(downward, wait_send))


def finish(tracer_ref, basis_ref, moments_ref, tracer_out, heights_out, heights, save):
    levels = tracer_ref.shape[0]
    saves = [pltpu.make_async_copy(tracer_ref.at[k], tracer_out.at[k], save.at[k]) for k in range(levels)]
    for copy in saves:
        copy.start()
    diag = iota((SUB, LANE), 1) == iota((SUB, LANE), 0)
    total = jnp.broadcast_to(moments_ref[...], (SUB, LANE))
    total = jnp.sum(jnp.where(diag, total, 0.0), axis=1, keepdims=True)
    moment = [total[i : i + 1, :] for i in range(2 * ITERS)]

    def inner(a, b):
        return sum(x * y * moment[i + j] for i, x in enumerate(a) for j, y in enumerate(b))

    def ratio(top, bottom):
        good = bottom > 0.0
        return jnp.where(good, top / jnp.where(good, bottom, 1.0), 0.0)

    one, zero = jnp.ones((1, 1), jnp.float32), jnp.zeros((1, 1), jnp.float32)
    scaled, direction, height = [one], [one], [zero] * ITERS
    product_now = moment[0]
    for iteration in range(ITERS):
        low, high = direction + [zero], [zero] + direction
        applied = [a - b for a, b in zip(low, high)]
        step_size = ratio(product_now, inner(direction, applied))
        for i, x in enumerate(direction):
            height[i] = height[i] + step_size * x
        if iteration + 1 < ITERS:
            scaled = [a - step_size * b for a, b in zip(scaled + [zero], applied)]
            product_next = jnp.maximum(inner(scaled, scaled), 0.0)
            factor = ratio(product_next, product_now)
            direction = [a + factor * b for a, b in zip(scaled, low)]
            product_now = product_next
    for b in range(basis_ref.shape[1]):
        heights[:, LANE * b : LANE * (b + 1)] = sum(h * basis_ref[i, b] for i, h in enumerate(height))

    saves.append(pltpu.make_async_copy(heights, heights_out, save.at[levels]))
    saves[-1].start()
    for copy in saves:
        copy.wait()


def on_device(ny, nx, tracer, east_speed, north_speed, columns, thickness, surface_flux, helm):
    levels, rows, cols = tracer.shape
    hbm = pl.BlockSpec(memory_space=pl.ANY)
    vmem = pl.BlockSpec(memory_space=pltpu.VMEM)
    f32 = jnp.float32
    dma = pltpu.SemaphoreType.DMA
    blocks = cols // LANE
    tall = rows + 2 * SUB
    scratch = [
        pltpu.VMEM((3, levels, rows, cols), f32),
        pltpu.VMEM((rows, cols), jnp.int32),
        pltpu.VMEM((3, blocks + 1, tall + SUB, LANE), f32),
        pltpu.VMEM((5, tall, LANE), f32),
        *[pltpu.VMEM((rows, LANE), f32)] * 2,
        *[pltpu.VMEM((tall, LANE), f32)] * 2,
        *[pltpu.VMEM((levels, blocks, 2 * SUB, LANE), f32)] * 4,
        pltpu.VMEM((2, 5, levels, blocks, 2 * SUB, LANE), f32),
        pltpu.VMEM((rows, cols), f32),
        pltpu.VMEM((2, rows, cols), f32),
        pltpu.VMEM((2, 6, tall + SUB, LANE), f32),
        pltpu.VMEM((blocks + 1, tall, LANE), f32),
        pltpu.VMEM((blocks + 1, tall, LANE), f32),
        pltpu.VMEM((ITERS, blocks + 1, tall + SUB, LANE), f32),
        pltpu.VMEM((1, LANE), f32),
        pltpu.VMEM((ny * nx - 1, 1, LANE), f32),
        pltpu.SMEM((levels,), f32),
        pltpu.SemaphoreType.REGULAR((max(ny, nx).bit_length(),)),
        dma((8 + 2 * blocks,)),
        dma((8,)),
        dma((8,)),
        dma,
        dma,
    ]
    results = pl.pallas_call(
        functools.partial(kernel, ny, nx),
        out_shape=(
            pltpu.VMEM((levels, rows, cols), f32),
            pltpu.VMEM((ITERS, blocks, rows, LANE), f32),
            pltpu.VMEM((1, LANE), f32),
        ),
        in_specs=[hbm] * 7,
        out_specs=(vmem,) * 3,
        scratch_shapes=scratch,
        compiler_params=pltpu.CompilerParams(collective_id=0, has_side_effects=True),
    )(tracer, east_speed, north_speed, columns, thickness, surface_flux, helm)
    return pl.pallas_call(
        finish,
        out_shape=(
            jax.ShapeDtypeStruct((levels, rows, cols), f32),
            jax.ShapeDtypeStruct((rows, cols), f32),
        ),
        in_specs=[vmem] * 3,
        out_specs=(hbm, hbm),
        scratch_shapes=[pltpu.VMEM((rows, cols), f32), dma((levels + 1,))],
    )(*[pltpu.with_memory_space_constraint(r, pltpu.VMEM) for r in results])


def solution(mesh):
    spec = P(None, "gy", "gx")
    flat = P("gy", "gx")
    return jax.shard_map(
        functools.partial(on_device, mesh.shape["gy"], mesh.shape["gx"]),
        mesh=mesh,
        in_specs=(spec, spec, spec, flat, P(), flat, flat),
        out_specs=(spec, flat),
        check_vma=False,
    )
```

```python
import functools

import jax
import jax.numpy as jnp
from jax import lax
from jax.experimental import pallas as pl
from jax.experimental.pallas import tpu as pltpu
from jax.sharding import PartitionSpec as P

TSTEPS = 2
ITERS = 3
MESH = pl.DeviceIdType.MESH
SUB = 8
LANE = 128
SEAM = 16


def roll(array, shift, axis):
    shift = shift % array.shape[axis]
    return pltpu.roll(array, shift, axis) if shift else array


def iota(shape, dim):
    return lax.broadcasted_iota(jnp.int32, shape, dim)


def pick(array, lanes):
    return jnp.take_along_axis(array, lanes, axis=1, mode="promise_in_bounds")


def transport(current, east, nort, open_east, open_nort):
    east = jnp.where(open_east, east, 0.0)
    nort = jnp.where(open_nort, nort, 0.0)
    for _ in range(TSTEPS):
        flux_east = east * jnp.where(east > 0.0, current, roll(current, -1, 1))
        flux_north = nort * jnp.where(nort > 0.0, current, roll(current, -1, 0))
        current = current - (flux_east - roll(flux_east, 1, 1) + flux_north - roll(flux_north, 1, 0))
    return current


def kernel(
    ny,
    nx,
    tracer_ref,
    east_ref,
    north_ref,
    columns_ref,
    thick_hbm,
    surface_ref,
    helm_ref,
    tracer_out,
    basis_out,
    moments_out,
    fields,
    col_in,
    flat,
    own_tile,
    to_east,
    to_west,
    west,
    east,
    rows_up,
    rows_down,
    rows_south,
    rows_north,
    row_strips,
    own_sum,
    faces,
    strips,
    level_sum,
    scale,
    start_vec,
    part,
    slots,
    thickness,
    know_sem,
    in_sem,
    send_sem,
    recv_sem,
    sum_send_sem,
    sum_recv_sem,
):
    _, levels, rows, cols = fields.shape
    my_y, my_x = lax.axis_index("gy"), lax.axis_index("gx")

    def wrap(value, size):
        return jnp.where(value >= size, value - size, value)

    ys = [my_y] + [wrap(my_y + d, ny) for d in range(1, ny)]
    xs = [my_x] + [wrap(my_x + d, nx) for d in range(1, nx)]
    others = [(y, x) for b, x in enumerate(xs) for a, y in enumerate(ys) if a or b]
    south_here, north_here = my_y > 0, my_y < ny - 1

    blocks = range(cols // LANE)
    side_block = cols // LANE
    inside = pl.ds(SUB, rows)
    small = [pltpu.make_async_copy(columns_ref, col_in, in_sem.at[0])] + [
        pltpu.make_async_copy(ref.at[:, pl.ds(LANE * b, LANE)], flat.at[f, b, inside], in_sem.at[1 + len(blocks) * (f - 1) + b])
        for f, ref in ((1, helm_ref), (2, surface_ref))
        for b in blocks
    ]
    halves = [range(0, levels // 2), range(levels // 2, levels)]
    large = [
        [
            pltpu.make_async_copy(
                ref.at[pl.ds(half[0], len(half))],
                fields.at[f, pl.ds(half[0], len(half))],
                in_sem.at[1 + 2 * len(blocks) + 2 * f + h],
            )
            for h, half in enumerate(halves)
        ]
        for f, ref in enumerate((tracer_ref, east_ref, north_ref))
    ]
    thick = pltpu.make_async_copy(thick_hbm, thickness, in_sem.at[7 + 2 * len(blocks)])
    for load in small + sum(large, []) + [thick]:
        load.start()
    barrier = pltpu.get_barrier_semaphore()

    def around(reach_y, reach_x):
        return [(ys[a], xs[b]) for a in reach_y for b in reach_x if a or b]

    def reach(distance, known, size):
        return (0,) if 2 * known + 1 >= size else (distance, -distance, 0)

    greeted = around(reach(1, 0, ny), reach(1, 0, nx))
    for target in greeted:
        pl.semaphore_signal(barrier, inc=1, device_id=target, device_id_type=MESH)
    rounds, known = [], 1
    while 2 * known + 1 < max(ny, nx):
        rounds.append(around(reach(known, known, ny), reach(known, known, nx)))
        known *= 2

    def tell(turn):
        for target in rounds[turn]:
            pl.semaphore_signal(know_sem.at[turn], inc=1, device_id=target, device_id_type=MESH)

    def hear(turn):
        pl.semaphore_wait(know_sem.at[turn], len(rounds[turn]))


    lane = iota((rows, LANE), 1)
    group = lane // SEAM
    seat = lane % SEAM
    first_rows, last_rows = pl.ds(0, SUB), pl.ds(rows - SUB, SUB)
    low_halo, low_own, high_own, high_halo = (pl.ds(at, SUB) for at in (0, SUB, rows, rows + SUB))

    def both_edges(left, right):
        return jnp.where(lane < LANE // 2, left, right)

    def flat_edges(f):
        return both_edges(flat[f, 0, inside], flat[f, side_block - 1, inside])

    def spare_lane(slot):
        return SEAM * (slot // 2) + SEAM - 2 + slot % 2

    for load in small:
        load.wait()
    for b in blocks:
        flat[0, b, inside] = col_in[:, LANE * b : LANE * (b + 1)].astype(jnp.float32)
    depth_edge = flat_edges(0)
    own_tile[3, inside] = pick(depth_edge, (LANE - SUB + seat) % LANE)
    three = jnp.where(
        (lane < SUB) | (lane >= LANE - SUB),
        depth_edge,
        jnp.where(lane < 3 * SUB, roll(flat_edges(1), 2 * SUB, 1), roll(flat_edges(2), 4 * SUB, 1)),
    )
    slot = jnp.maximum(2 * group + seat - (SEAM - 2), 0)
    east_from = jnp.where(slot < 6, LANE - 5 + slot, jnp.where(slot < 10, slot - 6 + 13, slot - 10 + 29)) % LANE
    west_from = jnp.where(slot < 6, slot, jnp.where(slot < 10, slot - 6 + 16, slot - 10 + 32)) % LANE
    spare_east, spare_west = pick(three, east_from), pick(three, west_from)
    sub = iota((SUB, LANE), 0)
    spare_up = ((0, -1), (0, -3), (0, -5), (1, -3), (1, -5), (2, -3), (2, -5))
    spare_down = ((0, 5), (0, 2), (1, 5), (2, 5))

    def spare_rows(which, k, b, where):
        field, turn = which[min(k, len(which) - 1)]
        return roll(flat[field, b, where], turn, 0)

    def pack_rows(k):
        for b in blocks:
            here = slice(LANE * b, LANE * (b + 1))
            c, e, n = (fields[f, k, rows - SUB : rows, here] for f in range(3))
            rows_up[k, b, 0:SUB] = jnp.where(sub < 3, roll(n, -3, 0), c)
            rows_up[k, b, SUB : 2 * SUB] = jnp.where(
                sub < 2, roll(n, 2, 0), jnp.where(sub < 4, spare_rows(spare_up, k, b, high_own), e)
            )
            c, e, n = (fields[f, k, 0:SUB, here] for f in range(3))
            rows_down[k, b, 0:SUB] = jnp.where(sub < 5, c, roll(n, 5, 0))
            rows_down[k, b, SUB : 2 * SUB] = jnp.where(
                sub < 4, e, jnp.where(sub < 5, roll(n, 1, 0), spare_rows(spare_down, k, b, low_own))
            )

    starts = (0, 5, 10, SEAM - 2)
    for f, (shift_east, shift_west) in enumerate(((-3, -8), (2, -3), (6, 2))):
        packed = None
        for h, half in enumerate(halves):
            large[f][h].wait()
            for k in half:
                both = both_edges(fields[f, k, :, 0:LANE], fields[f, k, :, cols - LANE : cols])
                moved = roll(both, SEAM * k + SUB, 1)
                packed = moved if packed is None else jnp.where(group == k, moved, packed)
            if f == 2:
                for k in half:
                    pack_rows(k)
        own_tile[f, inside] = packed
        seats = (seat >= starts[f]) & (seat < starts[f + 1])
        to_east[...] = jnp.where(seats, roll(packed, shift_east, 1), spare_east if f == 0 else to_east[...])
        to_west[...] = jnp.where(seats, roll(packed, shift_west, 1), spare_west if f == 0 else to_west[...])

    pl.semaphore_wait(barrier, len(greeted))

    up, down, right, left = wrap(my_y + 1, ny), wrap(my_y + ny - 1, ny), xs[1], xs[-1]
    plan = [
        (to_east, west.at[inside], (my_y, right)),
        (to_west, east.at[inside], (my_y, left)),
        (rows_up, rows_south, (up, my_x)),
        (to_east.at[last_rows], west.at[low_halo], (up, right)),
        (to_west.at[last_rows], east.at[low_halo], (up, left)),
        (rows_down, rows_north, (down, my_x)),
        (to_east.at[first_rows], west.at[high_halo], (down, right)),
        (to_west.at[first_rows], east.at[high_halo], (down, left)),
    ]
    copies = [
        pltpu.make_async_remote_copy(
            src_ref=source,
            dst_ref=target,
            send_sem=send_sem.at[which],
            recv_sem=recv_sem.at[which],
            device_id=device,
            device_id_type=MESH,
        )
        for which, (source, target, device) in enumerate(plan)
    ]
    beside, upward, downward = copies[0:2], copies[2:5], copies[5:8]

    def each(items, act):
        for item in items:
            act(item)

    start, wait_recv, wait_send = (lambda c: c.start()), (lambda c: c.wait_recv()), (lambda c: c.wait_send())
    far_east, far_west = my_x == nx - 1, my_x == 0
    pl.when(north_here)(lambda: each(upward[1:], start))
    pl.when(south_here)(lambda: each(downward[1:], start))
    pl.when(far_east)(copies[0].start)
    pl.when(far_west)(copies[1].start)
    far_up, far_down = my_y == ny // 2 - 1, my_y == ny // 2
    pl.when(far_up)(upward[0].start)
    pl.when(far_down)(downward[0].start)
    if rounds:
        tell(0)

    thick.wait()
    depth = col_in[...].astype(jnp.float32)
    faces[0] = jnp.minimum(depth, roll(depth, -1, 1))
    faces[1] = jnp.minimum(depth, roll(depth, -1, 0))
    own_sum[...] = jnp.zeros((rows, cols), jnp.float32)

    def level(k, carry):
        below = lax.convert_element_type(k, jnp.float32)
        current = transport(fields[0, k], fields[1, k], fields[2, k], faces[0] > below, faces[1] > below)
        tracer_out[k] = current
        own_sum[...] += jnp.where(col_in[...] > k, thickness[k] * current, 0.0)
        return carry

    part_way = levels * 1 // 8
    lax.fori_loop(0, part_way, level, 0, unroll=2)
    pl.when(north_here & jnp.logical_not(far_up))(upward[0].start)
    pl.when(south_here & jnp.logical_not(far_down))(downward[0].start)
    pl.when(jnp.logical_not(far_east))(copies[0].start)
    pl.when(jnp.logical_not(far_west))(copies[1].start)
    lax.fori_loop(part_way, levels, level, 0, unroll=2)

    def blank(rows_ref, halo):
        rows_ref[...] = jnp.zeros(rows_ref.shape, jnp.float32)
        for ref in (west, east):
            ref[halo] = jnp.zeros((SUB, LANE), jnp.float32)

    pl.when(jnp.logical_not(south_here))(lambda: blank(rows_south, low_halo))
    pl.when(jnp.logical_not(north_here))(lambda: blank(rows_north, high_halo))

    for turn in range(1, len(rounds)):
        hear(turn - 1)
        tell(turn)
    pl.when(south_here)(lambda: each(upward[:1], wait_recv))
    pl.when(north_here)(lambda: each(downward[:1], wait_recv))

    def at(start):
        return slice(start, start + SUB)

    lane = iota((SUB, LANE), 1)
    group = lane // SEAM
    seat = lane % SEAM
    low_half = lane < LANE // 2

    def beyond(values, step):
        turned = [roll(v, -step, 1) for v in values]
        near = lane < LANE - 1 if step > 0 else lane > 0
        return [jnp.where(near, t, turned[(b + step) % len(values)]) for b, t in enumerate(turned)]

    def receive_south(k):
        for b in blocks:
            first, second = rows_south[k, b, 0:SUB], rows_south[k, b, SUB : 2 * SUB]
            yield first, second, jnp.where(sub < 6, roll(first, 3, 0), roll(second, -2, 0))

    def receive_north(k):
        for b in blocks:
            first, second = rows_north[k, b, 0:SUB], rows_north[k, b, SUB : 2 * SUB]
            yield first, second, jnp.where(sub < 3, roll(first, -5, 0), roll(second, -1, 0))

    for b in blocks:
        spare = [rows_south[k, b, SUB : 2 * SUB] for k in range(7)]
        flat[0, b, low_halo] = jnp.where(
            sub < 5, roll(spare[0], 1, 0), jnp.where(sub < 7, roll(spare[1], 3, 0), roll(spare[2], 5, 0))
        )
        for f in (1, 2):
            flat[f, b, low_halo] = jnp.where(sub < 7, roll(spare[2 * f + 1], 3, 0), roll(spare[2 * f + 2], 5, 0))
        spare = [rows_north[k, b, SUB : 2 * SUB] for k in range(4)]
        flat[0, b, high_halo] = jnp.where(sub < 3, roll(spare[0], -5, 0), roll(spare[1], -2, 0))
        for f in (1, 2):
            flat[f, b, high_halo] = roll(spare[f + 1], -5, 0)
        scale[b] = 1.0 / (6.0 + flat[1, b, 0 : rows + 2 * SUB])
    depth_lanes = (LANE - SUB + seat) % LANE
    for halo in (low_halo, high_halo):
        own_tile[3, halo] = pick(jnp.where(low_half, flat[0, 0, halo], flat[0, side_block - 1, halo]), depth_lanes)
    for r in range(0, rows + 2 * SUB, SUB):
        own_tile[4, at(r)] = roll(own_tile[3, at(r)], -1, 1)

    row_sides = ((0, receive_south, 0, SUB, 0, low_halo), (1, receive_north, SUB, 0, rows, high_halo))
    for w, receive, halo_at, own_at, base, halo in row_sides:
        open_east, open_nort = [], []
        for r in (0, SUB):
            deep = [flat[0, b, at(base + r)] for b in blocks]
            open_east.append([jnp.minimum(d, e) for d, e in zip(deep, beyond(deep, 1))])
            ahead = [flat[0, b, at(base + r + 1)] for b in blocks]
            open_nort.append([jnp.minimum(d, a) for d, a in zip(deep, ahead)])
        packed = [None] * 3
        own_rows = pl.ds(0, SUB) if w == 0 else pl.ds(rows - SUB, SUB)
        for k in range(levels):
            got = list(receive(k))
            for f in range(3):
                moved = roll(jnp.where(low_half, got[0][f], got[-1][f]), SEAM * k + SUB, 1)
                packed[f] = moved if packed[f] is None else jnp.where(group == k, moved, packed[f])
            for b in blocks:
                for r, values in (
                    (halo_at, got[b]),
                    (own_at, [fields[f, k, own_rows, LANE * b : LANE * (b + 1)] for f in range(3)]),
                ):
                    t = r // SUB
                    row_strips[w, 0, k, b, at(r)] = values[0]
                    row_strips[w, 1, k, b, at(r)] = jnp.where(open_east[t][b] > k, values[1], 0.0)
                    row_strips[w, 2, k, b, at(r)] = jnp.where(open_nort[t][b] > k, values[2], 0.0)
        for f in range(3):
            own_tile[f, halo] = packed[f]

    def row_step(w, f, k, r):
        here, ahead, behind = ([row_strips[w, f, k, b, at(r + d)] for b in blocks] for d in (0, 1, -1))
        fast_east, fast_north = ([row_strips[w, g, k, b, at(r)] for b in blocks] for g in (1, 2))
        fast_south = [row_strips[w, 2, k, b, at(r - 1)] for b in blocks]
        flux_east = [v * jnp.where(v > 0.0, c, x) for v, c, x in zip(fast_east, here, beyond(here, 1))]
        out = []
        for b, flux_west in enumerate(beyond(flux_east, -1)):
            flux_north = fast_north[b] * jnp.where(fast_north[b] > 0.0, here[b], ahead[b])
            flux_south = fast_south[b] * jnp.where(fast_south[b] > 0.0, behind[b], here[b])
            out.append(here[b] - (flux_east[b] - flux_west + flux_north - flux_south))
        return out

    for k in range(levels):
        for w in range(2):
            for b, new in enumerate(row_step(w, 0, k, SUB - 4)):
                row_strips[w, 3, k, b, at(SUB - 4)] = new
    row_sums = [[jnp.zeros((SUB, LANE), jnp.float32) for _ in blocks] for _ in range(2)]
    for k in range(levels):
        for w, base in enumerate((0, rows)):
            for b, new in enumerate(row_step(w, 3, k, SUB - 3)):
                row_strips[w, 4, k, b, at(SUB - 3)] = new
                row_sums[w][b] += jnp.where(flat[0, b, at(base + SUB - 3)] > k, thickness[k] * new, 0.0)
    for b in blocks:
        level_sum[b, inside] = own_sum[:, LANE * b : LANE * (b + 1)]
        level_sum[b, SUB - 3 : SUB + 2] = row_sums[0][b][0:5]
        level_sum[b, rows + SUB - 2 : rows + SUB + 3] = row_sums[1][b][1:6]

    strip_level = group.astype(jnp.float32)
    lane_thickness = jnp.zeros((SUB, LANE), jnp.float32)
    for k in range(levels):
        lane_thickness = jnp.where(group == k, thickness[k], lane_thickness)
    def side_lanes(base_west, base_east):
        return spare_lane(jnp.where(low_half, base_east + (lane & 3), base_west + ((lane - (LANE - 3)) & 3)))

    side_pick = [side_lanes(*bases) for bases in ((2, 0), (6, 6), (10, 10))]
    sides = []
    for got, shifts, first, in_halo in (
        (west, (3, -2, -6), 3, [seat + d < SUB for d in (0, 1)]),
        (east, (8, 3, -2), 8, [seat + d >= SUB for d in (0, 1)]),
    ):
        depth_picks = [spare_lane(jnp.minimum(jnp.maximum(seat + d - first, 0), 4)) for d in (0, 1)]
        sides.append((got, shifts, depth_picks, in_halo))

    each(beside, wait_recv)
    pl.when(south_here)(lambda: each(upward[1:], wait_recv))
    pl.when(north_here)(lambda: each(downward[1:], wait_recv))

    tall_rows = range(0, rows + 2 * SUB, SUB)
    for w, (got, shifts, depth_picks, in_halo) in enumerate(sides):
        for d, lanes in enumerate(depth_picks):
            for r in tall_rows:
                strips[w, 3 + d, at(r)] = jnp.where(in_halo[d], pick(got[at(r)], lanes), own_tile[3 + d, at(r)])
    for f, lanes in enumerate(side_pick):
        for r in tall_rows:
            flat[f, side_block, at(r)] = jnp.where(low_half, pick(east[at(r)], lanes), pick(west[at(r)], lanes))
    for r in tall_rows:
        for w, (got, shifts, depth_picks, in_halo) in enumerate(sides):
            sent = got[at(r)]
            c, e, n = (jnp.where(in_halo[0], roll(sent, shift, 1), own_tile[f, at(r)]) for f, shift in enumerate(shifts))
            strips[w, 0, at(r)] = c
            strips[w, 1, at(r)] = jnp.where(jnp.minimum(strips[w, 3, at(r)], strips[w, 4, at(r)]) > strip_level, e, 0.0)
            strips[w, 2, at(r)] = n
    for r in range(0, rows + 2 * SUB, SUB):
        for w in range(2):
            open_nort = jnp.minimum(strips[w, 3, at(r)], strips[w, 3, at(r + 1)]) > strip_level
            strips[w, 2, at(r)] = jnp.where(open_nort, strips[w, 2, at(r)], 0.0)

    def side_step(w, f, r):
        here, ahead, behind = (strips[w, f, at(r + d)] for d in (0, 1, -1))
        fast_east, fast_north, fast_south = strips[w, 1, at(r)], strips[w, 2, at(r)], strips[w, 2, at(r - 1)]
        flux_east = fast_east * jnp.where(fast_east > 0.0, here, roll(here, -1, 1))
        flux_north = fast_north * jnp.where(fast_north > 0.0, here, ahead)
        flux_south = fast_south * jnp.where(fast_south > 0.0, behind, here)
        return here - (flux_east - roll(flux_east, 1, 1) + flux_north - flux_south)

    for r in range(SUB - 4, rows + SUB + 4, SUB):
        for w in range(2):
            strips[w, 4, at(r)] = side_step(w, 0, r)
    inner_rows = range(SUB - 3, rows + SUB + 3, SUB)
    for r in inner_rows:
        for w in range(2):
            new = side_step(w, 4, r)
            strips[w, 5, at(r)] = new
            strips[w, 0, at(r)] = jnp.where(strips[w, 3, at(r)] > strip_level, lane_thickness * new, 0.0)
    for r in inner_rows:
        for w in range(2):
            total = strips[w, 0, at(r)]
            strips[w, 1, at(r)] = total + roll(total, LANE // 2, 1)
    for r in inner_rows:
        for w in range(2):
            total = strips[w, 1, at(r)]
            strips[w, 2, at(r)] = sum(roll(total, shift - SUB, 1) for shift in range(0, LANE // 2, SEAM))
    for r in inner_rows:
        sum_west, sum_east = strips[0, 2, at(r)], strips[1, 2, at(r)]
        for b in range(side_block + 1):
            if b < side_block:
                total, inverse = level_sum[b, at(r)], scale[b, at(r)]
                if b == 0:
                    total = jnp.where(lane < 2, sum_west, total)
                if b == side_block - 1:
                    total = jnp.where(lane >= LANE - 2, sum_east, total)
            else:
                total = jnp.where(low_half, sum_east, sum_west)
                inverse = 1.0 / (6.0 + flat[1, b, at(r)])
            z0 = (flat[2, b, at(r)] + total) * inverse
            if b < side_block:
                level_sum[b, at(r)] = z0
            wet = flat[0, b, at(r)] > 0.0
            scale[b, at(r)] = jnp.where(wet, inverse, 0.0)
            start_vec[0, b, at(r)] = jnp.where(wet, z0, 0.0)

    def off_diagonal(source, r, wanted):
        upright, mixed = [], []
        for b in range(side_block + 1):
            both = start_vec[source, b, at(r - 1)] + start_vec[source, b, at(r + 1)]
            upright.append(both)
            mixed.append(start_vec[source, b, at(r)] + 0.5 * both)
        ahead, behind = ([roll(m, d, 1) for m in mixed] for d in (-1, 1))
        out = []
        for b in range(wanted):
            after = jnp.where(lane < LANE - 1, ahead[b], ahead[(b + 1) % (side_block + 1)])
            before = jnp.where(lane > 0, behind[b], behind[b - 1])
            out.append(scale[b, at(r)] * (upright[b] + after + before))
        return out

    for power in (1, 2):
        for r in range(SUB - 3 + power, rows + SUB + 3 - power, SUB):
            for b, z in enumerate(off_diagonal(power - 1, r, side_block + 1)):
                start_vec[power, b, at(r)] = z

    sums = [jnp.zeros((SUB, LANE), jnp.float32)] * (2 * ITERS)
    for r in range(SUB, rows + SUB, SUB):
        for b, z3 in enumerate(off_diagonal(2, r, side_block)):
            z = [level_sum[b, at(r)], start_vec[1, b, at(r)], start_vec[2, b, at(r)], z3]
            for i in range(ITERS):
                basis_out[i, b, at(r - SUB)] = z[i]
                scaled = (6.0 + flat[1, b, at(r)]) * z[i]
                sums[2 * i] += scaled * z[i]
                sums[2 * i + 1] += scaled * z[i + 1]
    sums = [jnp.sum(total, axis=0, keepdims=True) for total in sums]
    folded = jnp.concatenate(sums + [jnp.zeros((SUB - len(sums), LANE), jnp.float32)], axis=0)
    diag = iota((SUB, LANE), 1) == iota((SUB, LANE), 0)
    folded = jnp.sum(folded, axis=1, keepdims=True)
    part[...] = jnp.sum(jnp.where(diag, folded, 0.0), axis=0, keepdims=True)

    if rounds:
        hear(len(rounds) - 1)
    for index, target in reversed(list(enumerate(others))):
        pltpu.make_async_remote_copy(
            src_ref=part,
            dst_ref=slots.at[index],
            send_sem=sum_send_sem,
            recv_sem=sum_recv_sem,
            device_id=target,
            device_id_type=MESH,
        ).start()

    for k in range(levels):
        for b in blocks:
            here = slice(LANE * b, LANE * (b + 1))
            tracer_out[k, 0:2, here] = row_strips[0, 4, k, b, SUB : SUB + 2]
            tracer_out[k, rows - 2 : rows, here] = row_strips[1, 4, k, b, SUB - 2 : SUB]
    lane = iota((rows, LANE), 1)
    side_new = jnp.where(lane % SEAM < SUB, strips[1, 5, inside], strips[0, 5, inside])
    for k in range(levels):
        moved = roll(side_new, -SEAM * k - SUB, 1)
        tracer_out[k, :, 0:LANE] = jnp.where(lane < 2, moved, tracer_out[k, :, 0:LANE])
        tracer_out[k, :, cols - LANE : cols] = jnp.where(lane >= LANE - 2, moved, tracer_out[k, :, cols - LANE : cols])

    everything = pltpu.make_async_remote_copy(
        src_ref=slots,
        dst_ref=slots,
        send_sem=sum_send_sem,
        recv_sem=sum_recv_sem,
        device_id=others[0],
        device_id_type=MESH,
    )
    everything.wait_send()
    each(beside, wait_send)
    pl.when(north_here)(lambda: each(upward, wait_send))
    pl.when(south_here)(lambda: each(downward, wait_send))
    everything.wait_recv()
    moments_out[...] = jnp.sum(slots[...], axis=0) + part[...]


def finish(tracer_ref, basis_ref, moments_ref, tracer_out, heights_out, heights, save):
    levels = tracer_ref.shape[0]
    saves = [pltpu.make_async_copy(tracer_ref.at[k], tracer_out.at[k], save.at[k]) for k in range(levels)]
    for copy in saves:
        copy.start()
    diag = iota((SUB, LANE), 1) == iota((SUB, LANE), 0)
    total = jnp.broadcast_to(moments_ref[...], (SUB, LANE))
    total = jnp.sum(jnp.where(diag, total, 0.0), axis=1, keepdims=True)
    moment = [total[i : i + 1, :] for i in range(2 * ITERS)]

    def inner(a, b):
        return sum(x * y * moment[i + j] for i, x in enumerate(a) for j, y in enumerate(b))

    def ratio(top, bottom):
        good = bottom > 0.0
        return jnp.where(good, top / jnp.where(good, bottom, 1.0), 0.0)

    one, zero = jnp.ones((1, 1), jnp.float32), jnp.zeros((1, 1), jnp.float32)
    scaled, direction, height = [one], [one], [zero] * ITERS
    product_now = moment[0]
    for iteration in range(ITERS):
        low, high = direction + [zero], [zero] + direction
        applied = [a - b for a, b in zip(low, high)]
        step_size = ratio(product_now, inner(direction, applied))
        for i, x in enumerate(direction):
            height[i] = height[i] + step_size * x
        if iteration + 1 < ITERS:
            scaled = [a - step_size * b for a, b in zip(scaled + [zero], applied)]
            product_next = jnp.maximum(inner(scaled, scaled), 0.0)
            factor = ratio(product_next, product_now)
            direction = [a + factor * b for a, b in zip(scaled, low)]
            product_now = product_next
    for b in range(basis_ref.shape[1]):
        heights[:, LANE * b : LANE * (b + 1)] = sum(h * basis_ref[i, b] for i, h in enumerate(height))

    saves.append(pltpu.make_async_copy(heights, heights_out, save.at[levels]))
    saves[-1].start()
    for copy in saves:
        copy.wait()


def on_device(ny, nx, tracer, east_speed, north_speed, columns, thickness, surface_flux, helm):
    levels, rows, cols = tracer.shape
    hbm = pl.BlockSpec(memory_space=pl.ANY)
    vmem = pl.BlockSpec(memory_space=pltpu.VMEM)
    f32 = jnp.float32
    dma = pltpu.SemaphoreType.DMA
    blocks = cols // LANE
    tall = rows + 2 * SUB
    scratch = [
        pltpu.VMEM((3, levels, rows, cols), f32),
        pltpu.VMEM((rows, cols), jnp.int32),
        pltpu.VMEM((3, blocks + 1, tall + SUB, LANE), f32),
        pltpu.VMEM((5, tall, LANE), f32),
        *[pltpu.VMEM((rows, LANE), f32)] * 2,
        *[pltpu.VMEM((tall, LANE), f32)] * 2,
        *[pltpu.VMEM((levels, blocks, 2 * SUB, LANE), f32)] * 4,
        pltpu.VMEM((2, 5, levels, blocks, 2 * SUB, LANE), f32),
        pltpu.VMEM((rows, cols), f32),
        pltpu.VMEM((2, rows, cols), f32),
        pltpu.VMEM((2, 6, tall + SUB, LANE), f32),
        pltpu.VMEM((blocks + 1, tall, LANE), f32),
        pltpu.VMEM((blocks + 1, tall, LANE), f32),
        pltpu.VMEM((ITERS, blocks + 1, tall + SUB, LANE), f32),
        pltpu.VMEM((1, LANE), f32),
        pltpu.VMEM((ny * nx - 1, 1, LANE), f32),
        pltpu.SMEM((levels,), f32),
        pltpu.SemaphoreType.REGULAR((max(ny, nx).bit_length(),)),
        dma((8 + 2 * blocks,)),
        dma((8,)),
        dma((8,)),
        dma,
        dma,
    ]
    results = pl.pallas_call(
        functools.partial(kernel, ny, nx),
        out_shape=(
            pltpu.VMEM((levels, rows, cols), f32),
            pltpu.VMEM((ITERS, blocks, rows, LANE), f32),
            pltpu.VMEM((1, LANE), f32),
        ),
        in_specs=[hbm] * 7,
        out_specs=(vmem,) * 3,
        scratch_shapes=scratch,
        compiler_params=pltpu.CompilerParams(collective_id=0, has_side_effects=True),
    )(tracer, east_speed, north_speed, columns, thickness, surface_flux, helm)
    return pl.pallas_call(
        finish,
        out_shape=(
            jax.ShapeDtypeStruct((levels, rows, cols), f32),
            jax.ShapeDtypeStruct((rows, cols), f32),
        ),
        in_specs=[vmem] * 3,
        out_specs=(hbm, hbm),
        scratch_shapes=[pltpu.VMEM((rows, cols), f32), dma((levels + 1,))],
    )(*[pltpu.with_memory_space_constraint(r, pltpu.VMEM) for r in results])


def solution(mesh):
    spec = P(None, "gy", "gx")
    flat = P("gy", "gx")
    return jax.shard_map(
        functools.partial(on_device, mesh.shape["gy"], mesh.shape["gx"]),
        mesh=mesh,
        in_specs=(spec, spec, spec, flat, P(), flat, flat),
        out_specs=(spec, flat),
        check_vma=False,
    )
```

```python
import functools

import jax
import jax.numpy as jnp
from jax import lax
from jax.experimental import pallas as pl
from jax.experimental.pallas import tpu as pltpu
from jax.sharding import PartitionSpec as P

TSTEPS = 2
ITERS = 3
MESH = pl.DeviceIdType.MESH
SUB = 8
LANE = 128
SEAM = 16


def roll(array, shift, axis):
    shift = shift % array.shape[axis]
    return pltpu.roll(array, shift, axis) if shift else array


def iota(shape, dim):
    return lax.broadcasted_iota(jnp.int32, shape, dim)


def pick(array, lanes):
    return jnp.take_along_axis(array, lanes, axis=1, mode="promise_in_bounds")


def transport(current, east, nort, open_east, open_nort):
    east = jnp.where(open_east, east, 0.0)
    nort = jnp.where(open_nort, nort, 0.0)
    for _ in range(TSTEPS):
        flux_east = east * jnp.where(east > 0.0, current, roll(current, -1, 1))
        flux_north = nort * jnp.where(nort > 0.0, current, roll(current, -1, 0))
        current = current - (flux_east - roll(flux_east, 1, 1) + flux_north - roll(flux_north, 1, 0))
    return current


def kernel(
    ny,
    nx,
    tracer_ref,
    east_ref,
    north_ref,
    columns_ref,
    thick_hbm,
    surface_ref,
    helm_ref,
    tracer_out,
    basis_out,
    moments_out,
    fields,
    col_in,
    flat,
    own_tile,
    to_east,
    to_west,
    west,
    east,
    rows_up,
    rows_down,
    rows_south,
    rows_north,
    row_strips,
    own_sum,
    faces,
    strips,
    level_sum,
    scale,
    start_vec,
    part,
    slots,
    thickness,
    know_sem,
    in_sem,
    send_sem,
    recv_sem,
    sum_send_sem,
    sum_recv_sem,
):
    _, levels, rows, cols = fields.shape
    my_y, my_x = lax.axis_index("gy"), lax.axis_index("gx")

    def wrap(value, size):
        return jnp.where(value >= size, value - size, value)

    ys = [my_y] + [wrap(my_y + d, ny) for d in range(1, ny)]
    xs = [my_x] + [wrap(my_x + d, nx) for d in range(1, nx)]
    others = [(y, x) for b, x in enumerate(xs) for a, y in enumerate(ys) if a or b]
    south_here, north_here = my_y > 0, my_y < ny - 1

    blocks = range(cols // LANE)
    side_block = cols // LANE
    inside = pl.ds(SUB, rows)
    small = [pltpu.make_async_copy(columns_ref, col_in, in_sem.at[0])] + [
        pltpu.make_async_copy(ref.at[:, pl.ds(LANE * b, LANE)], flat.at[f, b, inside], in_sem.at[1 + len(blocks) * (f - 1) + b])
        for f, ref in ((1, helm_ref), (2, surface_ref))
        for b in blocks
    ]
    halves = [range(0, levels // 2), range(levels // 2, levels)]
    large = [
        [
            pltpu.make_async_copy(
                ref.at[pl.ds(half[0], len(half))],
                fields.at[f, pl.ds(half[0], len(half))],
                in_sem.at[1 + 2 * len(blocks) + 2 * f + h],
            )
            for h, half in enumerate(halves)
        ]
        for f, ref in enumerate((tracer_ref, east_ref, north_ref))
    ]
    thick = pltpu.make_async_copy(thick_hbm, thickness, in_sem.at[7 + 2 * len(blocks)])
    for load in small + sum(large, []) + [thick]:
        load.start()
    barrier = pltpu.get_barrier_semaphore()

    def around(reach_y, reach_x):
        return [(ys[a], xs[b]) for a in reach_y for b in reach_x if a or b]

    def reach(distance, known, size):
        return (0,) if 2 * known + 1 >= size else (distance, -distance, 0)

    greeted = around(reach(1, 0, ny), reach(1, 0, nx))
    for target in greeted:
        pl.semaphore_signal(barrier, inc=1, device_id=target, device_id_type=MESH)
    rounds, known = [], 1
    while 2 * known + 1 < max(ny, nx):
        rounds.append(around(reach(known, known, ny), reach(known, known, nx)))
        known *= 2

    def tell(turn):
        for target in rounds[turn]:
            pl.semaphore_signal(know_sem.at[turn], inc=1, device_id=target, device_id_type=MESH)

    def hear(turn):
        pl.semaphore_wait(know_sem.at[turn], len(rounds[turn]))


    lane = iota((rows, LANE), 1)
    group = lane // SEAM
    seat = lane % SEAM
    first_rows, last_rows = pl.ds(0, SUB), pl.ds(rows - SUB, SUB)
    low_halo, low_own, high_own, high_halo = (pl.ds(at, SUB) for at in (0, SUB, rows, rows + SUB))

    def both_edges(left, right):
        return jnp.where(lane < LANE // 2, left, right)

    def flat_edges(f):
        return both_edges(flat[f, 0, inside], flat[f, side_block - 1, inside])

    def spare_lane(slot):
        return SEAM * (slot // 2) + SEAM - 2 + slot % 2

    for load in small:
        load.wait()
    for b in blocks:
        flat[0, b, inside] = col_in[:, LANE * b : LANE * (b + 1)].astype(jnp.float32)
    depth_edge = flat_edges(0)
    own_tile[3, inside] = pick(depth_edge, (LANE - SUB + seat) % LANE)
    three = jnp.where(
        (lane < SUB) | (lane >= LANE - SUB),
        depth_edge,
        jnp.where(lane < 3 * SUB, roll(flat_edges(1), 2 * SUB, 1), roll(flat_edges(2), 4 * SUB, 1)),
    )
    slot = jnp.maximum(2 * group + seat - (SEAM - 2), 0)
    east_from = jnp.where(slot < 6, LANE - 5 + slot, jnp.where(slot < 10, slot - 6 + 13, slot - 10 + 29)) % LANE
    west_from = jnp.where(slot < 6, slot, jnp.where(slot < 10, slot - 6 + 16, slot - 10 + 32)) % LANE
    spare_east, spare_west = pick(three, east_from), pick(three, west_from)
    sub = iota((SUB, LANE), 0)
    spare_up = ((0, -1), (0, -3), (0, -5), (1, -3), (1, -5), (2, -3), (2, -5))
    spare_down = ((0, 5), (0, 2), (1, 5), (2, 5))

    def spare_rows(which, k, b, where):
        field, turn = which[min(k, len(which) - 1)]
        return roll(flat[field, b, where], turn, 0)

    def pack_rows(k):
        for b in blocks:
            here = slice(LANE * b, LANE * (b + 1))
            c, e, n = (fields[f, k, rows - SUB : rows, here] for f in range(3))
            rows_up[k, b, 0:SUB] = jnp.where(sub < 3, roll(n, -3, 0), c)
            rows_up[k, b, SUB : 2 * SUB] = jnp.where(
                sub < 2, roll(n, 2, 0), jnp.where(sub < 4, spare_rows(spare_up, k, b, high_own), e)
            )
            c, e, n = (fields[f, k, 0:SUB, here] for f in range(3))
            rows_down[k, b, 0:SUB] = jnp.where(sub < 5, c, roll(n, 5, 0))
            rows_down[k, b, SUB : 2 * SUB] = jnp.where(
                sub < 4, e, jnp.where(sub < 5, roll(n, 1, 0), spare_rows(spare_down, k, b, low_own))
            )

    starts = (0, 5, 10, SEAM - 2)
    for f, (shift_east, shift_west) in enumerate(((-3, -8), (2, -3), (6, 2))):
        packed = None
        for h, half in enumerate(halves):
            large[f][h].wait()
            for k in half:
                both = both_edges(fields[f, k, :, 0:LANE], fields[f, k, :, cols - LANE : cols])
                moved = roll(both, SEAM * k + SUB, 1)
                packed = moved if packed is None else jnp.where(group == k, moved, packed)
            if f == 2:
                for k in half:
                    pack_rows(k)
        own_tile[f, inside] = packed
        seats = (seat >= starts[f]) & (seat < starts[f + 1])
        to_east[...] = jnp.where(seats, roll(packed, shift_east, 1), spare_east if f == 0 else to_east[...])
        to_west[...] = jnp.where(seats, roll(packed, shift_west, 1), spare_west if f == 0 else to_west[...])

    pl.semaphore_wait(barrier, len(greeted))

    up, down, right, left = wrap(my_y + 1, ny), wrap(my_y + ny - 1, ny), xs[1], xs[-1]
    plan = [
        (to_east, west.at[inside], (my_y, right)),
        (to_west, east.at[inside], (my_y, left)),
        (rows_up, rows_south, (up, my_x)),
        (to_east.at[last_rows], west.at[low_halo], (up, right)),
        (to_west.at[last_rows], east.at[low_halo], (up, left)),
        (rows_down, rows_north, (down, my_x)),
        (to_east.at[first_rows], west.at[high_halo], (down, right)),
        (to_west.at[first_rows], east.at[high_halo], (down, left)),
    ]
    copies = [
        pltpu.make_async_remote_copy(
            src_ref=source,
            dst_ref=target,
            send_sem=send_sem.at[which],
            recv_sem=recv_sem.at[which],
            device_id=device,
            device_id_type=MESH,
        )
        for which, (source, target, device) in enumerate(plan)
    ]
    beside, upward, downward = copies[0:2], copies[2:5], copies[5:8]

    def each(items, act):
        for item in items:
            act(item)

    start, wait_recv, wait_send = (lambda c: c.start()), (lambda c: c.wait_recv()), (lambda c: c.wait_send())
    far_east, far_west = my_x == nx - 1, my_x == 0
    pl.when(north_here)(lambda: each(upward[1:], start))
    pl.when(south_here)(lambda: each(downward[1:], start))
    pl.when(far_east)(copies[0].start)
    pl.when(far_west)(copies[1].start)
    far_up, far_down = my_y == ny // 2 - 1, my_y == ny // 2
    pl.when(far_up)(upward[0].start)
    pl.when(far_down)(downward[0].start)
    if rounds:
        tell(0)

    thick.wait()
    depth = col_in[...].astype(jnp.float32)
    faces[0] = jnp.minimum(depth, roll(depth, -1, 1))
    faces[1] = jnp.minimum(depth, roll(depth, -1, 0))
    own_sum[...] = jnp.zeros((rows, cols), jnp.float32)

    def level(k, carry):
        below = lax.convert_element_type(k, jnp.float32)
        current = transport(fields[0, k], fields[1, k], fields[2, k], faces[0] > below, faces[1] > below)
        tracer_out[k] = current
        own_sum[...] += jnp.where(col_in[...] > k, thickness[k] * current, 0.0)
        return carry

    part_way = levels * 1 // 8
    lax.fori_loop(0, part_way, level, 0, unroll=2)
    pl.when(north_here & jnp.logical_not(far_up))(upward[0].start)
    pl.when(south_here & jnp.logical_not(far_down))(downward[0].start)
    pl.when(jnp.logical_not(far_east))(copies[0].start)
    pl.when(jnp.logical_not(far_west))(copies[1].start)
    lax.fori_loop(part_way, levels, level, 0, unroll=2)

    def blank(rows_ref, halo):
        rows_ref[...] = jnp.zeros(rows_ref.shape, jnp.float32)
        for ref in (west, east):
            ref[halo] = jnp.zeros((SUB, LANE), jnp.float32)

    pl.when(jnp.logical_not(south_here))(lambda: blank(rows_south, low_halo))
    pl.when(jnp.logical_not(north_here))(lambda: blank(rows_north, high_halo))

    for turn in range(1, len(rounds)):
        hear(turn - 1)
        tell(turn)
    pl.when(south_here)(lambda: each(upward[:1], wait_recv))
    pl.when(north_here)(lambda: each(downward[:1], wait_recv))

    def at(start):
        return slice(start, start + SUB)

    lane = iota((SUB, LANE), 1)
    group = lane // SEAM
    seat = lane % SEAM
    low_half = lane < LANE // 2

    def beyond(values, step):
        turned = [roll(v, -step, 1) for v in values]
        near = lane < LANE - 1 if step > 0 else lane > 0
        return [jnp.where(near, t, turned[(b + step) % len(values)]) for b, t in enumerate(turned)]

    def receive_south(k):
        for b in blocks:
            first, second = rows_south[k, b, 0:SUB], rows_south[k, b, SUB : 2 * SUB]
            yield first, second, jnp.where(sub < 6, roll(first, 3, 0), roll(second, -2, 0))

    def receive_north(k):
        for b in blocks:
            first, second = rows_north[k, b, 0:SUB], rows_north[k, b, SUB : 2 * SUB]
            yield first, second, jnp.where(sub < 3, roll(first, -5, 0), roll(second, -1, 0))

    for b in blocks:
        spare = [rows_south[k, b, SUB : 2 * SUB] for k in range(7)]
        flat[0, b, low_halo] = jnp.where(
            sub < 5, roll(spare[0], 1, 0), jnp.where(sub < 7, roll(spare[1], 3, 0), roll(spare[2], 5, 0))
        )
        for f in (1, 2):
            flat[f, b, low_halo] = jnp.where(sub < 7, roll(spare[2 * f + 1], 3, 0), roll(spare[2 * f + 2], 5, 0))
        spare = [rows_north[k, b, SUB : 2 * SUB] for k in range(4)]
        flat[0, b, high_halo] = jnp.where(sub < 3, roll(spare[0], -5, 0), roll(spare[1], -2, 0))
        for f in (1, 2):
            flat[f, b, high_halo] = roll(spare[f + 1], -5, 0)
        scale[b] = 1.0 / (6.0 + flat[1, b, 0 : rows + 2 * SUB])
    depth_lanes = (LANE - SUB + seat) % LANE
    for halo in (low_halo, high_halo):
        own_tile[3, halo] = pick(jnp.where(low_half, flat[0, 0, halo], flat[0, side_block - 1, halo]), depth_lanes)
    for r in range(0, rows + 2 * SUB, SUB):
        own_tile[4, at(r)] = roll(own_tile[3, at(r)], -1, 1)

    row_sides = ((0, receive_south, 0, SUB, 0, low_halo), (1, receive_north, SUB, 0, rows, high_halo))
    for w, receive, halo_at, own_at, base, halo in row_sides:
        open_east, open_nort = [], []
        for r in (0, SUB):
            deep = [flat[0, b, at(base + r)] for b in blocks]
            open_east.append([jnp.minimum(d, e) for d, e in zip(deep, beyond(deep, 1))])
            ahead = [flat[0, b, at(base + r + 1)] for b in blocks]
            open_nort.append([jnp.minimum(d, a) for d, a in zip(deep, ahead)])
        packed = [None] * 3
        own_rows = pl.ds(0, SUB) if w == 0 else pl.ds(rows - SUB, SUB)
        for k in range(levels):
            got = list(receive(k))
            for f in range(3):
                moved = roll(jnp.where(low_half, got[0][f], got[-1][f]), SEAM * k + SUB, 1)
                packed[f] = moved if packed[f] is None else jnp.where(group == k, moved, packed[f])
            for b in blocks:
                for r, values in (
                    (halo_at, got[b]),
                    (own_at, [fields[f, k, own_rows, LANE * b : LANE * (b + 1)] for f in range(3)]),
                ):
                    t = r // SUB
                    row_strips[w, 0, k, b, at(r)] = values[0]
                    row_strips[w, 1, k, b, at(r)] = jnp.where(open_east[t][b] > k, values[1], 0.0)
                    row_strips[w, 2, k, b, at(r)] = jnp.where(open_nort[t][b] > k, values[2], 0.0)
        for f in range(3):
            own_tile[f, halo] = packed[f]

    def row_step(w, f, k, r):
        here, ahead, behind = ([row_strips[w, f, k, b, at(r + d)] for b in blocks] for d in (0, 1, -1))
        fast_east, fast_north = ([row_strips[w, g, k, b, at(r)] for b in blocks] for g in (1, 2))
        fast_south = [row_strips[w, 2, k, b, at(r - 1)] for b in blocks]
        flux_east = [v * jnp.where(v > 0.0, c, x) for v, c, x in zip(fast_east, here, beyond(here, 1))]
        out = []
        for b, flux_west in enumerate(beyond(flux_east, -1)):
            flux_north = fast_north[b] * jnp.where(fast_north[b] > 0.0, here[b], ahead[b])
            flux_south = fast_south[b] * jnp.where(fast_south[b] > 0.0, behind[b], here[b])
            out.append(here[b] - (flux_east[b] - flux_west + flux_north - flux_south))
        return out

    for k in range(levels):
        for w in range(2):
            for b, new in enumerate(row_step(w, 0, k, SUB - 4)):
                row_strips[w, 3, k, b, at(SUB - 4)] = new
    row_sums = [[jnp.zeros((SUB, LANE), jnp.float32) for _ in blocks] for _ in range(2)]
    for k in range(levels):
        for w, base in enumerate((0, rows)):
            for b, new in enumerate(row_step(w, 3, k, SUB - 3)):
                row_strips[w, 4, k, b, at(SUB - 3)] = new
                row_sums[w][b] += jnp.where(flat[0, b, at(base + SUB - 3)] > k, thickness[k] * new, 0.0)
    for b in blocks:
        level_sum[b, inside] = own_sum[:, LANE * b : LANE * (b + 1)]
        level_sum[b, SUB - 3 : SUB + 2] = row_sums[0][b][0:5]
        level_sum[b, rows + SUB - 2 : rows + SUB + 3] = row_sums[1][b][1:6]

    strip_level = group.astype(jnp.float32)
    lane_thickness = jnp.zeros((SUB, LANE), jnp.float32)
    for k in range(levels):
        lane_thickness = jnp.where(group == k, thickness[k], lane_thickness)
    def side_lanes(base_west, base_east):
        return spare_lane(jnp.where(low_half, base_east + (lane & 3), base_west + ((lane - (LANE - 3)) & 3)))

    side_pick = [side_lanes(*bases) for bases in ((2, 0), (6, 6), (10, 10))]
    sides = []
    for got, shifts, first, in_halo in (
        (west, (3, -2, -6), 3, [seat + d < SUB for d in (0, 1)]),
        (east, (8, 3, -2), 8, [seat + d >= SUB for d in (0, 1)]),
    ):
        depth_picks = [spare_lane(jnp.minimum(jnp.maximum(seat + d - first, 0), 4)) for d in (0, 1)]
        sides.append((got, shifts, depth_picks, in_halo))

    each(beside, wait_recv)

    def unpack(tall_rows):
        for w, (got, shifts, depth_picks, in_halo) in enumerate(sides):
            for d, lanes in enumerate(depth_picks):
                for r in tall_rows:
                    strips[w, 3 + d, at(r)] = jnp.where(in_halo[d], pick(got[at(r)], lanes), own_tile[3 + d, at(r)])
        for f, lanes in enumerate(side_pick):
            for r in tall_rows:
                flat[f, side_block, at(r)] = jnp.where(low_half, pick(east[at(r)], lanes), pick(west[at(r)], lanes))
        for r in tall_rows:
            for w, (got, shifts, depth_picks, in_halo) in enumerate(sides):
                sent = got[at(r)]
                c, e, n = (jnp.where(in_halo[0], roll(sent, shift, 1), own_tile[f, at(r)]) for f, shift in enumerate(shifts))
                strips[w, 0, at(r)] = c
                strips[w, 1, at(r)] = jnp.where(jnp.minimum(strips[w, 3, at(r)], strips[w, 4, at(r)]) > strip_level, e, 0.0)
                strips[w, 2, at(r)] = n

    unpack(range(SUB, rows + SUB, SUB))
    pl.when(south_here)(lambda: each(upward[1:], wait_recv))
    pl.when(north_here)(lambda: each(downward[1:], wait_recv))
    unpack((0, rows + SUB))
    for r in range(0, rows + 2 * SUB, SUB):
        for w in range(2):
            open_nort = jnp.minimum(strips[w, 3, at(r)], strips[w, 3, at(r + 1)]) > strip_level
            strips[w, 2, at(r)] = jnp.where(open_nort, strips[w, 2, at(r)], 0.0)

    def side_step(w, f, r):
        here, ahead, behind = (strips[w, f, at(r + d)] for d in (0, 1, -1))
        fast_east, fast_north, fast_south = strips[w, 1, at(r)], strips[w, 2, at(r)], strips[w, 2, at(r - 1)]
        flux_east = fast_east * jnp.where(fast_east > 0.0, here, roll(here, -1, 1))
        flux_north = fast_north * jnp.where(fast_north > 0.0, here, ahead)
        flux_south = fast_south * jnp.where(fast_south > 0.0, behind, here)
        return here - (flux_east - roll(flux_east, 1, 1) + flux_north - flux_south)

    for r in range(SUB - 4, rows + SUB + 4, SUB):
        for w in range(2):
            strips[w, 4, at(r)] = side_step(w, 0, r)
    inner_rows = range(SUB - 3, rows + SUB + 3, SUB)
    for r in inner_rows:
        for w in range(2):
            new = side_step(w, 4, r)
            strips[w, 5, at(r)] = new
            strips[w, 0, at(r)] = jnp.where(strips[w, 3, at(r)] > strip_level, lane_thickness * new, 0.0)
    for r in inner_rows:
        for w in range(2):
            total = strips[w, 0, at(r)]
            strips[w, 1, at(r)] = total + roll(total, LANE // 2, 1)
    for r in inner_rows:
        for w in range(2):
            total = strips[w, 1, at(r)]
            strips[w, 2, at(r)] = sum(roll(total, shift - SUB, 1) for shift in range(0, LANE // 2, SEAM))
    for r in inner_rows:
        sum_west, sum_east = strips[0, 2, at(r)], strips[1, 2, at(r)]
        for b in range(side_block + 1):
            if b < side_block:
                total, inverse = level_sum[b, at(r)], scale[b, at(r)]
                if b == 0:
                    total = jnp.where(lane < 2, sum_west, total)
                if b == side_block - 1:
                    total = jnp.where(lane >= LANE - 2, sum_east, total)
            else:
                total = jnp.where(low_half, sum_east, sum_west)
                inverse = 1.0 / (6.0 + flat[1, b, at(r)])
            z0 = (flat[2, b, at(r)] + total) * inverse
            if b < side_block:
                level_sum[b, at(r)] = z0
            wet = flat[0, b, at(r)] > 0.0
            scale[b, at(r)] = jnp.where(wet, inverse, 0.0)
            start_vec[0, b, at(r)] = jnp.where(wet, z0, 0.0)

    def off_diagonal(source, r, wanted):
        upright, mixed = [], []
        for b in range(side_block + 1):
            both = start_vec[source, b, at(r - 1)] + start_vec[source, b, at(r + 1)]
            upright.append(both)
            mixed.append(start_vec[source, b, at(r)] + 0.5 * both)
        ahead, behind = ([roll(m, d, 1) for m in mixed] for d in (-1, 1))
        out = []
        for b in range(wanted):
            after = jnp.where(lane < LANE - 1, ahead[b], ahead[(b + 1) % (side_block + 1)])
            before = jnp.where(lane > 0, behind[b], behind[b - 1])
            out.append(scale[b, at(r)] * (upright[b] + after + before))
        return out

    for power in (1, 2):
        for r in range(SUB - 3 + power, rows + SUB + 3 - power, SUB):
            for b, z in enumerate(off_diagonal(power - 1, r, side_block + 1)):
                start_vec[power, b, at(r)] = z

    sums = [jnp.zeros((SUB, LANE), jnp.float32)] * (2 * ITERS)
    for r in range(SUB, rows + SUB, SUB):
        for b, z3 in enumerate(off_diagonal(2, r, side_block)):
            z = [level_sum[b, at(r)], start_vec[1, b, at(r)], start_vec[2, b, at(r)], z3]
            for i in range(ITERS):
                basis_out[i, b, at(r - SUB)] = z[i]
                scaled = (6.0 + flat[1, b, at(r)]) * z[i]
                sums[2 * i] += scaled * z[i]
                sums[2 * i + 1] += scaled * z[i + 1]
    sums = [jnp.sum(total, axis=0, keepdims=True) for total in sums]
    folded = jnp.concatenate(sums + [jnp.zeros((SUB - len(sums), LANE), jnp.float32)], axis=0)
    diag = iota((SUB, LANE), 1) == iota((SUB, LANE), 0)
    folded = jnp.sum(folded, axis=1, keepdims=True)
    part[...] = jnp.sum(jnp.where(diag, folded, 0.0), axis=0, keepdims=True)

    if rounds:
        hear(len(rounds) - 1)
    for index, target in reversed(list(enumerate(others))):
        pltpu.make_async_remote_copy(
            src_ref=part,
            dst_ref=slots.at[index],
            send_sem=sum_send_sem,
            recv_sem=sum_recv_sem,
            device_id=target,
            device_id_type=MESH,
        ).start()

    for k in range(levels):
        for b in blocks:
            here = slice(LANE * b, LANE * (b + 1))
            tracer_out[k, 0:2, here] = row_strips[0, 4, k, b, SUB : SUB + 2]
            tracer_out[k, rows - 2 : rows, here] = row_strips[1, 4, k, b, SUB - 2 : SUB]
    lane = iota((rows, LANE), 1)
    side_new = jnp.where(lane % SEAM < SUB, strips[1, 5, inside], strips[0, 5, inside])
    for k in range(levels):
        moved = roll(side_new, -SEAM * k - SUB, 1)
        tracer_out[k, :, 0:LANE] = jnp.where(lane < 2, moved, tracer_out[k, :, 0:LANE])
        tracer_out[k, :, cols - LANE : cols] = jnp.where(lane >= LANE - 2, moved, tracer_out[k, :, cols - LANE : cols])

    everything = pltpu.make_async_remote_copy(
        src_ref=slots,
        dst_ref=slots,
        send_sem=sum_send_sem,
        recv_sem=sum_recv_sem,
        device_id=others[0],
        device_id_type=MESH,
    )
    everything.wait_send()
    each(beside, wait_send)
    pl.when(north_here)(lambda: each(upward, wait_send))
    pl.when(south_here)(lambda: each(downward, wait_send))
    everything.wait_recv()
    moments_out[...] = jnp.sum(slots[...], axis=0) + part[...]


def finish(tracer_ref, basis_ref, moments_ref, tracer_out, heights_out, heights, save):
    levels = tracer_ref.shape[0]
    saves = [pltpu.make_async_copy(tracer_ref.at[k], tracer_out.at[k], save.at[k]) for k in range(levels)]
    for copy in saves:
        copy.start()
    diag = iota((SUB, LANE), 1) == iota((SUB, LANE), 0)
    total = jnp.broadcast_to(moments_ref[...], (SUB, LANE))
    total = jnp.sum(jnp.where(diag, total, 0.0), axis=1, keepdims=True)
    moment = [total[i : i + 1, :] for i in range(2 * ITERS)]

    def inner(a, b):
        return sum(x * y * moment[i + j] for i, x in enumerate(a) for j, y in enumerate(b))

    def ratio(top, bottom):
        good = bottom > 0.0
        return jnp.where(good, top / jnp.where(good, bottom, 1.0), 0.0)

    one, zero = jnp.ones((1, 1), jnp.float32), jnp.zeros((1, 1), jnp.float32)
    scaled, direction, height = [one], [one], [zero] * ITERS
    product_now = moment[0]
    for iteration in range(ITERS):
        low, high = direction + [zero], [zero] + direction
        applied = [a - b for a, b in zip(low, high)]
        step_size = ratio(product_now, inner(direction, applied))
        for i, x in enumerate(direction):
            height[i] = height[i] + step_size * x
        if iteration + 1 < ITERS:
            scaled = [a - step_size * b for a, b in zip(scaled + [zero], applied)]
            product_next = jnp.maximum(inner(scaled, scaled), 0.0)
            factor = ratio(product_next, product_now)
            direction = [a + factor * b for a, b in zip(scaled, low)]
            product_now = product_next
    for b in range(basis_ref.shape[1]):
        heights[:, LANE * b : LANE * (b + 1)] = sum(h * basis_ref[i, b] for i, h in enumerate(height))

    saves.append(pltpu.make_async_copy(heights, heights_out, save.at[levels]))
    saves[-1].start()
    for copy in saves:
        copy.wait()


def on_device(ny, nx, tracer, east_speed, north_speed, columns, thickness, surface_flux, helm):
    levels, rows, cols = tracer.shape
    hbm = pl.BlockSpec(memory_space=pl.ANY)
    vmem = pl.BlockSpec(memory_space=pltpu.VMEM)
    f32 = jnp.float32
    dma = pltpu.SemaphoreType.DMA
    blocks = cols // LANE
    tall = rows + 2 * SUB
    scratch = [
        pltpu.VMEM((3, levels, rows, cols), f32),
        pltpu.VMEM((rows, cols), jnp.int32),
        pltpu.VMEM((3, blocks + 1, tall + SUB, LANE), f32),
        pltpu.VMEM((5, tall, LANE), f32),
        *[pltpu.VMEM((rows, LANE), f32)] * 2,
        *[pltpu.VMEM((tall, LANE), f32)] * 2,
        *[pltpu.VMEM((levels, blocks, 2 * SUB, LANE), f32)] * 4,
        pltpu.VMEM((2, 5, levels, blocks, 2 * SUB, LANE), f32),
        pltpu.VMEM((rows, cols), f32),
        pltpu.VMEM((2, rows, cols), f32),
        pltpu.VMEM((2, 6, tall + SUB, LANE), f32),
        pltpu.VMEM((blocks + 1, tall, LANE), f32),
        pltpu.VMEM((blocks + 1, tall, LANE), f32),
        pltpu.VMEM((ITERS, blocks + 1, tall + SUB, LANE), f32),
        pltpu.VMEM((1, LANE), f32),
        pltpu.VMEM((ny * nx - 1, 1, LANE), f32),
        pltpu.SMEM((levels,), f32),
        pltpu.SemaphoreType.REGULAR((max(ny, nx).bit_length(),)),
        dma((8 + 2 * blocks,)),
        dma((8,)),
        dma((8,)),
        dma,
        dma,
    ]
    results = pl.pallas_call(
        functools.partial(kernel, ny, nx),
        out_shape=(
            pltpu.VMEM((levels, rows, cols), f32),
            pltpu.VMEM((ITERS, blocks, rows, LANE), f32),
            pltpu.VMEM((1, LANE), f32),
        ),
        in_specs=[hbm] * 7,
        out_specs=(vmem,) * 3,
        scratch_shapes=scratch,
        compiler_params=pltpu.CompilerParams(collective_id=0, has_side_effects=True),
    )(tracer, east_speed, north_speed, columns, thickness, surface_flux, helm)
    return pl.pallas_call(
        finish,
        out_shape=(
            jax.ShapeDtypeStruct((levels, rows, cols), f32),
            jax.ShapeDtypeStruct((rows, cols), f32),
        ),
        in_specs=[vmem] * 3,
        out_specs=(hbm, hbm),
        scratch_shapes=[pltpu.VMEM((rows, cols), f32), dma((levels + 1,))],
    )(*[pltpu.with_memory_space_constraint(r, pltpu.VMEM) for r in results])


def solution(mesh):
    spec = P(None, "gy", "gx")
    flat = P("gy", "gx")
    return jax.shard_map(
        functools.partial(on_device, mesh.shape["gy"], mesh.shape["gx"]),
        mesh=mesh,
        in_specs=(spec, spec, spec, flat, P(), flat, flat),
        out_specs=(spec, flat),
        check_vma=False,
    )
```
